128 devices in a mesh: rows: 4 (over y_hi, core), cols: 4 (over z), heads: 8 (over x, y_lo).
Axes of the slice: x: 4, y: 4 (y_hi: 2, y_lo: 2; y = y_hi * 2 + y_lo), z: 4, core: 2. Of those that a mesh axis runs over, the one named last changes fastest.
Arguments:
- tokens: bfloat16 [16384, 1024], P(('rows', 'cols'), 'heads'), may hold values from -8 to 8
- ln_gain: float32 [1024], replicated, may hold values from 0.1 to 1.9
- w_qkv: bfloat16 [3, 1024, 1024], P(None, None, 'heads'), may hold values from -1 to 1
- w_out: bfloat16 [1024, 1024], P('heads'), may hold values from -0.1875 to 0.1875
- out_bias: float32 [1024], P('heads'), may hold values from -3 to 3
Outputs:
- mixed: bfloat16 [16384, 1024], P(('rows', 'cols'), 'heads')
The draws below stay inside these ranges and needn't reach their ends.
All inputs are finite; a program needn't handle non-finite values.
Results may differ from the reference program's by a relative error of at most 0.0095.
Values may be sent and summed in bfloat16 or wider, within the bound.
No kernel may reach another device: no remote copies, remote signals or barrier semaphores. Data moves between devices by JAX's collectives and lax.ppermute only.
A program may use at most 64 MiB of HBM per device.

```python
import jax
import jax.numpy as jnp
from jax import lax

D = 1024
HEADS = 16
TOKENS = 16384
N_HEADS = 8


def draw_tokens(key, part):
    first = jax.random.fold_in(jax.random.fold_in(key, 3), 0)
    base = jax.random.normal(first, (TOKENS, D), jnp.float32)
    return jnp.clip(base, -8.0, 8.0).astype(jnp.bfloat16)


def draw_w_qkv(key, part):
    first = jax.random.fold_in(jax.random.fold_in(key, 5), 0)
    base = jax.random.normal(first, (3, D, D), jnp.float32) * D ** (-0.5)
    spread = jnp.array([1.7, 1.7, 1.0], jnp.float32).reshape(3, 1, 1)
    base = base * spread
    return jnp.clip(base, -1.0, 1.0).astype(jnp.bfloat16)


def block_scale(key, shape, cuts, least, top_value):
    gain, own = 1.0, jax.random.fold_in(key, 6)
    for position, blocks in cuts:
        draws = jnp.exp(jax.random.uniform(jax.random.fold_in(own, position), (blocks,), jnp.float32, least / len(cuts), top_value / len(cuts)))
        gain = gain * jnp.repeat(draws, shape[position] // blocks).reshape([-1 if axis == position else 1 for axis in range(len(shape))])
    return gain


def scatter_about(key, extent, width, reach, cuts=(), held_as=jnp.bfloat16):
    drawn = jax.random.normal(key, extent, jnp.float32) * width
    if len(cuts) > 0:
        drawn = block_scale(key, extent, cuts, -0.22, 0.18) * drawn
    return jnp.clip(drawn, min=-reach, max=reach).astype(held_as)


def setup_inputs(seed: int = 0) -> dict:
    key_of = jax.random.split(jax.random.key(seed), 6)
    tokens = draw_tokens(jax.random.fold_in(key_of[5], 71), 0)
    ln_gain = jnp.clip(1.0 + 0.18 * jax.random.normal(key_of[1], (D,), jnp.float32), 0.1, 1.9)
    w_qkv = draw_w_qkv(jax.random.fold_in(key_of[5], 71), 0)
    w_out = scatter_about(key_of[3], (D, D), D ** -0.5, 0.1875, ((0, 8),))
    out_bias = scatter_about(key_of[4], (D,), 0.5, 3.0, ((0, 8),), jnp.float32)
    return {"tokens": tokens, "ln_gain": ln_gain, "w_qkv": w_qkv, "w_out": w_out, "out_bias": out_bias}


def layer_norm(tokens, ln_gain):
    xf = tokens.astype(jnp.float32)
    mean = lax.optimization_barrier(jnp.mean(xf, axis=-1, keepdims=True))
    centered = xf - mean
    var = lax.optimization_barrier(jnp.mean(centered * centered, axis=-1, keepdims=True))
    return (centered * lax.rsqrt(var + 1e-06) * ln_gain).astype(jnp.bfloat16)

def reference(tokens, ln_gain, w_qkv, w_out, out_bias):
    normed = layer_norm(tokens, ln_gain)
    query = jnp.dot(normed, w_qkv[0], preferred_element_type=jnp.float32).astype(jnp.bfloat16)
    keys = jnp.dot(normed, w_qkv[1], preferred_element_type=jnp.float32).astype(jnp.bfloat16)
    values = jnp.dot(normed, w_qkv[2], preferred_element_type=jnp.float32).astype(jnp.bfloat16)
    head_dim = D // HEADS
    scale = 1.0 / head_dim ** 0.5
    block = 1024 if TOKENS % 1024 == 0 else TOKENS
    nblocks = TOKENS // block
    qt = query.reshape(TOKENS, HEADS, head_dim).transpose(1, 0, 2)
    kt = keys.reshape(TOKENS, HEADS, head_dim).transpose(1, 0, 2)
    vt = values.reshape(TOKENS, HEADS, head_dim).transpose(1, 0, 2)

    def one_head(args):
        qh, kh, vh = args

        def qblock(rows):
            scores = jnp.dot(rows, kh.T, preferred_element_type=jnp.float32) * scale
            peak = lax.optimization_barrier(jnp.max(scores, axis=-1, keepdims=True))
            weights = jnp.exp(scores - peak)
            den = lax.optimization_barrier(jnp.sum(weights, axis=-1, keepdims=True))
            num = jnp.dot(weights.astype(jnp.bfloat16), vh, preferred_element_type=jnp.float32)
            return num / den
        return lax.map(qblock, qh.reshape(nblocks, block, head_dim)).reshape(TOKENS, head_dim)
    attended = lax.map(one_head, (qt, kt, vt))
    attended = attended.transpose(1, 0, 2).reshape(TOKENS, D).astype(jnp.bfloat16)
    group = D // N_HEADS
    summed = jnp.zeros((TOKENS, D), jnp.float32)
    for index in range(N_HEADS):
        part = jnp.dot(attended[:, index * group:(index + 1) * group], w_out[index * group:(index + 1) * group], preferred_element_type=jnp.float32)
        part = lax.optimization_barrier(part.astype(jnp.bfloat16))
        summed = summed + part.astype(jnp.float32)
    return (tokens.astype(jnp.float32) + summed + out_bias).astype(jnp.bfloat16)
```

```python
import functools

import jax
import jax.numpy as jnp
from jax import lax
from jax.experimental import pallas as pl
from jax.experimental.pallas import tpu as pltpu
from jax.sharding import PartitionSpec as P

D = 1024
HEADS = 16
HD = 64
LOG2E = 1.4426950408889634
QSCALE = LOG2E / HD**0.5
CAP = 2.0**60
AXES = ("rows", "cols", "heads")
bf16 = jnp.bfloat16
f32 = jnp.float32


def perm(move):
    pairs = []
    for i in range(128):
        here = dict(x=(i % 8) // 2, yl=i % 2, z=(i // 8) % 4, yh=i // 64, c=(i // 32) % 2)
        to = {**here, **move(here)}
        pairs.append((i, ((to["yh"] * 2 + to["c"]) * 4 + to["z"]) * 8 + to["x"] * 2 + to["yl"]))
    return pairs


Z_UP = perm(lambda d: dict(z=(d["z"] + 1) % 4))
Z_DOWN = perm(lambda d: dict(z=(d["z"] - 1) % 4))
Z_FAR = perm(lambda d: dict(z=(d["z"] + 2) % 4))
YH_SWAP = perm(lambda d: dict(yh=1 - d["yh"]))
YL_SWAP = perm(lambda d: dict(yl=1 - d["yl"]))
CORE_SWAP = perm(lambda d: dict(c=1 - d["c"]))
X_GROUPS = [[0, 2, 4, 6], [1, 3, 5, 7]]


def send(x, pairs):
    return lax.ppermute(x, AXES, pairs)


def vmem():
    return pl.BlockSpec(memory_space=pltpu.VMEM)


def smem():
    return pl.BlockSpec(memory_space=pltpu.SMEM)


def project_kernel(par_ref, x_ref, gain_ref, w_ref, kv_ref, q_ref, out_ref, n_ref):
    tok = x_ref.shape[1]
    step = 128
    par = par_ref[0]
    lane = lax.broadcasted_iota(jnp.int32, (step, 128), 1)
    low = lane < HD

    def one(t, _):
        rows = pl.ds(pl.multiple_of(t * step, step), step)
        parts = [x_ref[h, rows, :].astype(f32) for h in range(8)]
        total = parts[0]
        for p in parts[1:]:
            total = total + p
        mean = jnp.sum(total, axis=1, keepdims=True) * (1.0 / D)
        sq = None
        for h in range(8):
            c = parts[h] - mean
            sq = c * c if sq is None else sq + c * c
        var = jnp.sum(sq, axis=1, keepdims=True) * (1.0 / D)
        inv = lax.rsqrt(var + 1e-06)
        for h in range(8):
            g = gain_ref[:, h * 128 : (h + 1) * 128]
            n_ref[:, h * 128 : (h + 1) * 128] = ((parts[h] - mean) * inv * g).astype(bf16)
        normed = n_ref[...]
        q = jnp.dot(normed, w_ref[0], preferred_element_type=f32) * QSCALE
        k = jnp.dot(normed, w_ref[1], preferred_element_type=f32)
        v = jnp.dot(normed, w_ref[2], preferred_element_type=f32)
        first = jnp.where(low, k, pltpu.roll(v, HD, 1))
        second = jnp.where(low, pltpu.roll(k, HD, 1), v)
        keep = jnp.where(par > 0, second, first)
        give = jnp.where(par > 0, first, second)
        kv_ref[rows, :] = keep.astype(bf16)
        out_ref[rows, :] = give.astype(bf16)
        qt = q.T
        qkeep = jnp.where(par > 0, qt[HD:], qt[:HD])
        qgive = jnp.where(par > 0, qt[:HD], qt[HD:])
        q_ref[pl.ds(pl.multiple_of(t * HD, HD), HD), :] = qkeep.astype(bf16)
        out_ref[pl.ds(pl.multiple_of(tok + t * HD, HD), HD), :] = qgive.astype(bf16)
        return 0

    lax.fori_loop(0, tok // step, one, 0)


def project(par, x, gain, w):
    tok = x.shape[1]
    return pl.pallas_call(
        project_kernel,
        out_shape=(
            jax.ShapeDtypeStruct((tok, 128), bf16),
            jax.ShapeDtypeStruct((tok // 2, 128), bf16),
            jax.ShapeDtypeStruct((tok + tok // 2, 128), bf16),
        ),
        in_specs=[smem(), vmem(), vmem(), vmem()],
        out_specs=(vmem(), vmem(), vmem()),
        scratch_shapes=[pltpu.VMEM((128, D), bf16)],
        compiler_params=pltpu.CompilerParams(vmem_limit_bytes=40 << 20),
        name="project",
    )(par, x, gain, w)


def attend_kernel(*refs, npieces, nq, first, last, bq, bk):
    pieces = refs[:npieces]
    qs = refs[npieces : npieces + nq]
    rest = list(refs[npieces + nq :])
    if not first:
        acc_in, m_in = rest[:2]
        rest = rest[2:]
    if last:
        out_ref = rest[0]
        rest = rest[1:]
        acc_ref, m_ref, kvs, vt, q2, s = rest
    else:
        acc_ref, m_ref, kvs, vt, q2, s = rest
    nkeys = kvs.shape[0]
    nkb = nkeys // bk
    nqb = q2.shape[0]
    base = 0
    vt[HD:, :] = jnp.ones((vt.shape[0] - HD, nkeys), bf16)
    for piece in pieces:
        count = piece.shape[0]

        def load(i, _, piece=piece, base=base):
            at = pl.multiple_of(i * 256, 256)
            to = pl.multiple_of(base + i * 256, 256)
            block = piece[pl.ds(at, 256), :]
            kvs[pl.ds(to, 256), :] = block
            vt[0:HD, pl.ds(to, 256)] = block.T[HD:, :]
            return 0

        lax.fori_loop(0, count // 256, load, 0)
        base += count
    per = bq // 128
    jb = 0
    for q in qs:
        for j in range(q.shape[0] // HD // per):
            for b in range(per):
                q2[jb, 0:HD, b * 128 : (b + 1) * 128] = q[(j * per + b) * HD : (j * per + b + 1) * HD, :]
            jb += 1
    q2[:, HD:, :] = jnp.zeros((nqb, HD, bq), bf16)

    def scores(j, i):
        return jnp.dot(kvs[pl.ds(pl.multiple_of(i * bk, bk), bk), :], q2[j], preferred_element_type=f32)

    def reset(j, _):
        if first:
            top = jnp.dot(kvs[0:256, :], q2[j], preferred_element_type=f32)
            m_ref[j] = jnp.max(top, axis=0, keepdims=True)
            acc_ref[j] = jnp.zeros(acc_ref.shape[1:], f32)
        else:
            m_ref[j] = m_in[j]
            acc_ref[j] = acc_in[j]
        return 0

    lax.fori_loop(0, nqb, reset, 0)

    steps = nqb * nkb

    def one(t, a, b):
        u = jnp.where(t + 1 < steps, t + 1, 0)
        s[b] = scores(u // nkb, u % nkb)
        j = t // nkb
        p = jnp.exp2(s[a] - m_ref[j]).astype(bf16)
        at = pl.ds(pl.multiple_of((t % nkb) * bk, bk), bk)
        acc_ref[j] += jnp.dot(vt[:, at], p, preferred_element_type=f32)

    def sweep():
        s[0] = scores(0, 0)

        def two(h, _):
            one(2 * h, 0, 1)
            one(2 * h + 1, 1, 0)
            return 0

        lax.fori_loop(0, steps // 2, two, 0)

    sweep()
    den = acc_ref[:, HD : HD + 1, :]
    fine = jnp.min(jnp.where(den < CAP, 1.0, 0.0)) > 0.5

    @pl.when(jnp.logical_not(fine))
    def _():
        def exact(j, _):
            def widen(i, top):
                return jnp.maximum(top, jnp.max(scores(j, i), axis=0, keepdims=True))

            if first:
                top = lax.fori_loop(0, nkb, widen, jnp.full((1, bq), -jnp.inf, f32))
                acc_ref[j] = jnp.zeros(acc_ref.shape[1:], f32)
            else:
                old = m_in[j]
                top = lax.fori_loop(0, nkb, widen, old)
                acc_ref[j] = acc_in[j] * jnp.exp2(old - top)
            m_ref[j] = top
            return 0

        lax.fori_loop(0, nqb, exact, 0)
        sweep()

    if last:
        def finish(j, _):
            a = acc_ref[j]
            o = (a[0:HD] / a[HD : HD + 1]).astype(bf16)
            for b in range(per):
                out_ref[pl.ds(pl.multiple_of((j * per + b) * HD, HD), HD), :] = o[:, b * 128 : (b + 1) * 128]
            return 0

        lax.fori_loop(0, nqb, finish, 0)


def attend(name, pieces, qs, state=None, last=False, bq=256, bk=1024):
    nkeys = sum(p.shape[0] for p in pieces)
    nqueries = sum(q.shape[0] for q in qs) * 2
    nqb = nqueries // bq
    acc_shape = (nqb, HD + 16, bq)
    m_shape = (nqb, 1, bq)
    scratch = [
        pltpu.VMEM((nkeys, 128), bf16),
        pltpu.VMEM((HD + 16, nkeys), bf16),
        pltpu.VMEM((nqb, 128, bq), bf16),
        pltpu.VMEM((2, bk, bq), f32),
    ]
    if last:
        out_shape = jax.ShapeDtypeStruct((nqueries // 2, 128), bf16)
        out_specs = vmem()
        scratch = [pltpu.VMEM(acc_shape, f32), pltpu.VMEM(m_shape, f32)] + scratch
    else:
        out_shape = (jax.ShapeDtypeStruct(acc_shape, f32), jax.ShapeDtypeStruct(m_shape, f32))
        out_specs = (vmem(), vmem())
    args = [*pieces, *qs] + ([] if state is None else list(state))
    flops = 4 * nkeys * nqueries * 128
    return pl.pallas_call(
        functools.partial(
            attend_kernel, npieces=len(pieces), nq=len(qs), first=state is None, last=last, bq=bq, bk=bk
        ),
        out_shape=out_shape,
        in_specs=[vmem()] * len(args),
        out_specs=out_specs,
        scratch_shapes=scratch,
        compiler_params=pltpu.CompilerParams(vmem_limit_bytes=48 << 20),
        cost_estimate=pl.CostEstimate(flops=flops, transcendentals=nkeys * nqueries, bytes_accessed=nkeys * 256),
        name=name,
    )(*args)


def mix_kernel(att_ref, w_ref, out_ref):
    blocks = att_ref.shape[1] // HD

    def one(t, _):
        at = pl.ds(pl.multiple_of(t * HD, HD), HD)
        cols = jnp.concatenate([att_ref[g, at, :] for g in range(4)], axis=0)
        rows = cols.T
        part = jnp.dot(rows, w_ref[...], preferred_element_type=f32).astype(bf16)
        for b in range(4):
            out_ref[b, pl.ds(pl.multiple_of(t * 128, 128), 128), :] = part[:, b * 128 : (b + 1) * 128]
        return 0

    lax.fori_loop(0, blocks, one, 0)


def mix(att, w):
    tok = att.shape[1] * 2
    return pl.pallas_call(
        mix_kernel,
        out_shape=jax.ShapeDtypeStruct((4, tok, 128), bf16),
        in_specs=[vmem(), vmem()],
        out_specs=vmem(),
        compiler_params=pltpu.CompilerParams(vmem_limit_bytes=32 << 20),
        name="mix",
    )(att, w)


def per_device(tokens, ln_gain, w_qkv, w_out, out_bias):
    rows = lax.axis_index("rows")
    heads = lax.axis_index("heads")
    yh = rows // 2
    yl = heads % 2
    tok = tokens.shape[0]
    par = yh.astype(jnp.int32).reshape(1)

    copies = jnp.broadcast_to(tokens, (8, *tokens.shape))
    whole = lax.all_to_all(copies, "heads", split_axis=0, concat_axis=0, tiled=True)
    wcols = w_out.reshape(128, 4, 2, 128)
    mine = jnp.where(yl > 0, wcols[:, :, 1], wcols[:, :, 0]).reshape(128, 512)
    theirs = jnp.where(yl > 0, wcols[:, :, 0], wcols[:, :, 1]).reshape(128, 512)
    other = send(theirs, YL_SWAP)

    kv, q, give = project(par, whole, ln_gain.reshape(1, D), w_qkv)
    got = send(give, YH_SWAP)
    q_far = got[tok:]
    near = jnp.concatenate([kv, got[:tok]], axis=0)
    near_other = send(near, CORE_SWAP)
    up = send(near, Z_UP)
    down = send(near, Z_DOWN)
    far = send(near, Z_FAR)
    qs = (q_far, q)
    state = attend("attend_near", (near, near_other), qs)
    up_other = send(up, CORE_SWAP)
    down_other = send(down, CORE_SWAP)
    state = attend("attend_ring", (up, down, up_other, down_other), qs, state)
    far_other = send(far, CORE_SWAP)
    acc, m = state
    half = acc.shape[0] // 2
    att_far = attend("attend_last_far", (far, far_other), (q_far,), (acc[:half], m[:half]), last=True)
    back = send(att_far, YH_SWAP)
    att = attend("attend_last_near", (far, far_other), (q,), (acc[half:], m[half:]), last=True)
    own = jnp.where(yh > 0, jnp.stack([back, att]), jnp.stack([att, back]))
    peer = send(own, YL_SWAP)
    att4 = jnp.concatenate([own, peer], axis=0)
    w4 = jnp.concatenate([mine, other], axis=0)
    part = mix(att4, w4)
    parts = lax.all_to_all(part, "heads", split_axis=0, concat_axis=0, axis_index_groups=X_GROUPS, tiled=True)
    summed = jnp.sum(parts.astype(f32), axis=0)
    return (tokens.astype(f32) + summed + out_bias).astype(bf16)


def solution(mesh):
    return jax.shard_map(
        per_device,
        mesh=mesh,
        in_specs=(
            P(("rows", "cols"), "heads"),
            P(),
            P(None, None, "heads"),
            P("heads", None),
            P("heads"),
        ),
        out_specs=P(("rows", "cols"), "heads"),
        check_vma=False,
    )
```

```python
import functools

import jax
import jax.numpy as jnp
from jax import lax
from jax.experimental import pallas as pl
from jax.experimental.pallas import tpu as pltpu
from jax.sharding import PartitionSpec as P

D = 1024
HEADS = 16
HD = 64
LOG2E = 1.4426950408889634
QSCALE = LOG2E / HD**0.5
CAP = 2.0**60
AXES = ("rows", "cols", "heads")
bf16 = jnp.bfloat16
f32 = jnp.float32


def perm(move):
    pairs = []
    for i in range(128):
        here = dict(x=(i % 8) // 2, yl=i % 2, z=(i // 8) % 4, yh=i // 64, c=(i // 32) % 2)
        to = {**here, **move(here)}
        pairs.append((i, ((to["yh"] * 2 + to["c"]) * 4 + to["z"]) * 8 + to["x"] * 2 + to["yl"]))
    return pairs


Z_UP = perm(lambda d: dict(z=(d["z"] + 1) % 4))
Z_DOWN = perm(lambda d: dict(z=(d["z"] - 1) % 4))
Z_FAR = perm(lambda d: dict(z=(d["z"] + 2) % 4))
YH_SWAP = perm(lambda d: dict(yh=1 - d["yh"]))
YL_SWAP = perm(lambda d: dict(yl=1 - d["yl"]))
CORE_SWAP = perm(lambda d: dict(c=1 - d["c"]))
X_UP = perm(lambda d: dict(x=(d["x"] + 1) % 4))
X_DOWN = perm(lambda d: dict(x=(d["x"] - 1) % 4))
X_FAR = perm(lambda d: dict(x=(d["x"] + 2) % 4))


def send(x, pairs):
    return lax.ppermute(x, AXES, pairs)


def vmem():
    return pl.BlockSpec(memory_space=pltpu.VMEM)


def smem():
    return pl.BlockSpec(memory_space=pltpu.SMEM)


def project_kernel(ids_ref, *refs):
    x_refs = refs[:8]
    gain_ref, w_ref, kv_ref, q_ref, out_ref, n_ref = refs[8:]
    tok = x_refs[0].shape[0]
    step = 128
    par = ids_ref[8]
    lane = lax.broadcasted_iota(jnp.int32, (step, 128), 1)
    low = lane < HD

    def one(t, _):
        rows = pl.ds(pl.multiple_of(t * step, step), step)
        parts = [x_ref[rows, :].astype(f32) for x_ref in x_refs]
        total = parts[0]
        for p in parts[1:]:
            total = total + p
        mean = jnp.sum(total, axis=1, keepdims=True) * (1.0 / D)
        sq = None
        for h in range(8):
            c = parts[h] - mean
            sq = c * c if sq is None else sq + c * c
        var = jnp.sum(sq, axis=1, keepdims=True) * (1.0 / D)
        inv = lax.rsqrt(var + 1e-06)
        for h in range(8):
            n_ref[ids_ref[h]] = ((parts[h] - mean) * inv * gain_ref[ids_ref[h]]).astype(bf16)
        normed = jnp.concatenate([n_ref[h] for h in range(8)], axis=1)
        q = jnp.dot(normed, w_ref[0], preferred_element_type=f32) * QSCALE
        k = jnp.dot(normed, w_ref[1], preferred_element_type=f32)
        v = jnp.dot(normed, w_ref[2], preferred_element_type=f32)
        first = jnp.where(low, k, pltpu.roll(v, HD, 1))
        second = jnp.where(low, pltpu.roll(k, HD, 1), v)
        keep = jnp.where(par > 0, second, first)
        give = jnp.where(par > 0, first, second)
        kv_ref[rows, :] = keep.astype(bf16)
        out_ref[rows, :] = give.astype(bf16)
        qt = q.T
        qkeep = jnp.where(par > 0, qt[HD:], qt[:HD])
        qgive = jnp.where(par > 0, qt[:HD], qt[HD:])
        q_ref[pl.ds(pl.multiple_of(t * HD, HD), HD), :] = qkeep.astype(bf16)
        out_ref[pl.ds(pl.multiple_of(tok + t * HD, HD), HD), :] = qgive.astype(bf16)
        return 0

    lax.fori_loop(0, tok // step, one, 0)


def project(ids, blocks, gain, w):
    tok = blocks[0].shape[0]
    return pl.pallas_call(
        project_kernel,
        out_shape=(
            jax.ShapeDtypeStruct((tok, 128), bf16),
            jax.ShapeDtypeStruct((tok // 2, 128), bf16),
            jax.ShapeDtypeStruct((tok + tok // 2, 128), bf16),
        ),
        in_specs=[smem()] + [vmem()] * 10,
        out_specs=(vmem(), vmem(), vmem()),
        scratch_shapes=[pltpu.VMEM((8, 128, 128), bf16)],
        compiler_params=pltpu.CompilerParams(vmem_limit_bytes=40 << 20),
        name="project",
    )(ids, *blocks, gain, w)


def attend_kernel(*refs, npieces, nq, first, last, bq, bk):
    pieces = refs[:npieces]
    qs = refs[npieces : npieces + nq]
    rest = list(refs[npieces + nq :])
    if not first:
        acc_in, m_in = rest[:2]
        rest = rest[2:]
    if last:
        out_ref = rest[0]
        rest = rest[1:]
        acc_ref, m_ref, kvs, vt, q2, s = rest
    else:
        acc_ref, m_ref, kvs, vt, q2, s = rest
    nkeys = kvs.shape[0]
    nkb = nkeys // bk
    nqb = q2.shape[0]
    base = 0
    vt[HD:, :] = jnp.ones((vt.shape[0] - HD, nkeys), bf16)
    for piece in pieces:
        count = piece.shape[0]

        def load(i, _, piece=piece, base=base):
            at = pl.multiple_of(i * 256, 256)
            to = pl.multiple_of(base + i * 256, 256)
            block = piece[pl.ds(at, 256), :]
            kvs[pl.ds(to, 256), :] = block
            vt[0:HD, pl.ds(to, 256)] = block.T[HD:, :]
            return 0

        lax.fori_loop(0, count // 256, load, 0)
        base += count
    per = bq // 128
    jb = 0
    for q in qs:
        for j in range(q.shape[0] // HD // per):
            for b in range(per):
                q2[jb, 0:HD, b * 128 : (b + 1) * 128] = q[(j * per + b) * HD : (j * per + b + 1) * HD, :]
            jb += 1
    q2[:, HD:, :] = jnp.zeros((nqb, HD, bq), bf16)

    def scores(j, i):
        return jnp.dot(kvs[pl.ds(pl.multiple_of(i * bk, bk), bk), :], q2[j], preferred_element_type=f32)

    def reset(j, _):
        if first:
            top = jnp.dot(kvs[0:256, :], q2[j], preferred_element_type=f32)
            m_ref[j] = jnp.max(top, axis=0, keepdims=True)
            acc_ref[j] = jnp.zeros(acc_ref.shape[1:], f32)
        else:
            m_ref[j] = m_in[j]
            acc_ref[j] = acc_in[j]
        return 0

    lax.fori_loop(0, nqb, reset, 0)

    steps = nqb * nkb

    def one(t, a, b):
        u = jnp.where(t + 1 < steps, t + 1, 0)
        s[b] = scores(u // nkb, u % nkb)
        j = t // nkb
        p = jnp.exp2(s[a] - m_ref[j]).astype(bf16)
        at = pl.ds(pl.multiple_of((t % nkb) * bk, bk), bk)
        acc_ref[j] += jnp.dot(vt[:, at], p, preferred_element_type=f32)

    def sweep():
        s[0] = scores(0, 0)

        def two(h, _):
            one(2 * h, 0, 1)
            one(2 * h + 1, 1, 0)
            return 0

        lax.fori_loop(0, steps // 2, two, 0)

    sweep()
    den = acc_ref[:, HD : HD + 1, :]
    fine = jnp.min(jnp.where(den < CAP, 1.0, 0.0)) > 0.5

    @pl.when(jnp.logical_not(fine))
    def _():
        def exact(j, _):
            def widen(i, top):
                return jnp.maximum(top, jnp.max(scores(j, i), axis=0, keepdims=True))

            if first:
                top = lax.fori_loop(0, nkb, widen, jnp.full((1, bq), -jnp.inf, f32))
                acc_ref[j] = jnp.zeros(acc_ref.shape[1:], f32)
            else:
                old = m_in[j]
                top = lax.fori_loop(0, nkb, widen, old)
                acc_ref[j] = acc_in[j] * jnp.exp2(old - top)
            m_ref[j] = top
            return 0

        lax.fori_loop(0, nqb, exact, 0)
        sweep()

    if last:
        def finish(j, _):
            a = acc_ref[j]
            o = (a[0:HD] / a[HD : HD + 1]).astype(bf16)
            for b in range(per):
                out_ref[pl.ds(pl.multiple_of((j * per + b) * HD, HD), HD), :] = o[:, b * 128 : (b + 1) * 128]
            return 0

        lax.fori_loop(0, nqb, finish, 0)


def attend(name, pieces, qs, state=None, last=False, bq=256, bk=1024):
    nkeys = sum(p.shape[0] for p in pieces)
    nqueries = sum(q.shape[0] for q in qs) * 2
    nqb = nqueries // bq
    acc_shape = (nqb, HD + 16, bq)
    m_shape = (nqb, 1, bq)
    scratch = [
        pltpu.VMEM((nkeys, 128), bf16),
        pltpu.VMEM((HD + 16, nkeys), bf16),
        pltpu.VMEM((nqb, 128, bq), bf16),
        pltpu.VMEM((2, bk, bq), f32),
    ]
    if last:
        out_shape = jax.ShapeDtypeStruct((nqueries // 2, 128), bf16)
        out_specs = vmem()
        scratch = [pltpu.VMEM(acc_shape, f32), pltpu.VMEM(m_shape, f32)] + scratch
    else:
        out_shape = (jax.ShapeDtypeStruct(acc_shape, f32), jax.ShapeDtypeStruct(m_shape, f32))
        out_specs = (vmem(), vmem())
    args = [*pieces, *qs] + ([] if state is None else list(state))
    flops = 4 * nkeys * nqueries * 128
    return pl.pallas_call(
        functools.partial(
            attend_kernel, npieces=len(pieces), nq=len(qs), first=state is None, last=last, bq=bq, bk=bk
        ),
        out_shape=out_shape,
        in_specs=[vmem()] * len(args),
        out_specs=out_specs,
        scratch_shapes=scratch,
        compiler_params=pltpu.CompilerParams(vmem_limit_bytes=48 << 20),
        cost_estimate=pl.CostEstimate(flops=flops, transcendentals=nkeys * nqueries, bytes_accessed=nkeys * 256),
        name=name,
    )(*args)


def mix_kernel(x_ref, *refs):
    att_refs = refs[:4]
    w_ref = refs[4]
    out_refs = refs[5:]
    x = x_ref[0]

    def one(t, _):
        at = pl.ds(pl.multiple_of(t * HD, HD), HD)
        rows = jnp.concatenate([a[at, :] for a in att_refs], axis=0).T
        to = pl.ds(pl.multiple_of(t * 128, 128), 128)
        for b in (0, 2):
            w = jnp.concatenate([w_ref[(x + b) % 4], w_ref[(x + b + 1) % 4]], axis=1)
            part = jnp.dot(rows, w, preferred_element_type=f32).astype(bf16)
            out_refs[b][to, :] = part[:, :128]
            out_refs[b + 1][to, :] = part[:, 128:]
        return 0

    lax.fori_loop(0, att_refs[0].shape[0] // HD, one, 0)


def mix(x, att, w):
    tok = att[0].shape[0] * 2
    return pl.pallas_call(
        mix_kernel,
        out_shape=[jax.ShapeDtypeStruct((tok, 128), bf16)] * 4,
        in_specs=[smem()] + [vmem()] * 5,
        out_specs=[vmem()] * 4,
        compiler_params=pltpu.CompilerParams(vmem_limit_bytes=32 << 20),
        name="mix",
    )(x, *att, w)


def per_device(tokens, ln_gain, w_qkv, w_out, out_bias):
    rows = lax.axis_index("rows")
    heads = lax.axis_index("heads")
    yh = rows // 2
    x = heads // 2
    yl = heads % 2
    tok = tokens.shape[0]

    by_y = send(tokens, YL_SWAP)
    by_up = send(tokens, X_UP)
    by_down = send(tokens, X_DOWN)
    by_y, by_up, by_down, again = lax.optimization_barrier((by_y, by_up, by_down, tokens))
    y_up = send(by_up, YL_SWAP)
    y_down = send(by_down, YL_SWAP)
    by_far = send(again, X_FAR)
    y_far = send(by_y, X_FAR)
    blocks = (tokens, by_up, by_down, by_far, by_y, y_up, y_down, y_far)
    xs = jnp.stack([x, (x + 3) % 4, (x + 1) % 4, (x + 2) % 4])
    ids = jnp.concatenate([xs * 2 + yl, xs * 2 + 1 - yl, yh.reshape(1)]).astype(jnp.int32)

    wcols = w_out.reshape(128, 4, 2, 128)
    mine = jnp.where(yl > 0, wcols[:, :, 1], wcols[:, :, 0]).transpose(1, 0, 2)
    theirs = jnp.where(yl > 0, wcols[:, :, 0], wcols[:, :, 1]).transpose(1, 0, 2)

    kv, q, give = project(ids, blocks, ln_gain.reshape(8, 1, 128), w_qkv)
    got = send(give, YH_SWAP)
    other = send(theirs, YL_SWAP)
    q_far = got[tok:]
    near = jnp.concatenate([kv, got[:tok]], axis=0)
    near_other = send(near, CORE_SWAP)
    up = send(near, Z_UP)
    down = send(near, Z_DOWN)
    far = send(near, Z_FAR)
    qs = (q_far, q)
    state = attend("attend_near", (near, near_other), qs)
    up, down, state = lax.optimization_barrier((up, down, state))
    up_other = send(up, CORE_SWAP)
    down_other = send(down, CORE_SWAP)
    state = attend("attend_ring", (up, down, up_other, down_other), qs, state)
    far, state = lax.optimization_barrier((far, state))
    far_other = send(far, CORE_SWAP)
    acc, m = state
    half = acc.shape[0] // 2
    att_far = attend("attend_last_far", (far, far_other), (q_far,), (acc[:half], m[:half]), last=True)
    back = send(att_far, YH_SWAP)
    att = attend("attend_last_near", (far, far_other), (q,), (acc[half:], m[half:]), last=True)
    peer_att = send(att, YL_SWAP)
    peer_back = send(back, YL_SWAP)
    att4 = [
        jnp.where(yh > 0, back, att),
        jnp.where(yh > 0, att, back),
        jnp.where(yh > 0, peer_back, peer_att),
        jnp.where(yh > 0, peer_att, peer_back),
    ]
    w4 = jnp.concatenate([mine, other], axis=1)
    part = mix(x.astype(jnp.int32).reshape(1), att4, w4)
    parts = [part[0], send(part[1], X_UP), send(part[2], X_FAR), send(part[3], X_DOWN)]
    summed = sum(p.astype(f32) for p in parts[1:]) + parts[0].astype(f32)
    return (tokens.astype(f32) + summed + out_bias).astype(bf16)


def solution(mesh):
    return jax.shard_map(
        per_device,
        mesh=mesh,
        in_specs=(
            P(("rows", "cols"), "heads"),
            P(),
            P(None, None, "heads"),
            P("heads", None),
            P("heads"),
        ),
        out_specs=P(("rows", "cols"), "heads"),
        check_vma=False,
    )
```

```python
import functools

import jax
import jax.numpy as jnp
from jax import lax
from jax.experimental import pallas as pl
from jax.experimental.pallas import tpu as pltpu
from jax.sharding import PartitionSpec as P

D = 1024
HEADS = 16
HD = 64
LOG2E = 1.4426950408889634
QSCALE = LOG2E / HD**0.5
CAP = 2.0**60
AXES = ("rows", "cols", "heads")
bf16 = jnp.bfloat16
f32 = jnp.float32


def perm(move):
    pairs = []
    for i in range(128):
        here = dict(x=(i % 8) // 2, yl=i % 2, z=(i // 8) % 4, yh=i // 64, c=(i // 32) % 2)
        to = {**here, **move(here)}
        pairs.append((i, ((to["yh"] * 2 + to["c"]) * 4 + to["z"]) * 8 + to["x"] * 2 + to["yl"]))
    return pairs


Z_UP = perm(lambda d: dict(z=(d["z"] + 1) % 4))
Z_DOWN = perm(lambda d: dict(z=(d["z"] - 1) % 4))
Z_FAR = perm(lambda d: dict(z=(d["z"] + 2) % 4))
YH_SWAP = perm(lambda d: dict(yh=1 - d["yh"]))
YL_SWAP = perm(lambda d: dict(yl=1 - d["yl"]))
CORE_SWAP = perm(lambda d: dict(c=1 - d["c"]))
X_UP = perm(lambda d: dict(x=(d["x"] + 1) % 4))
X_DOWN = perm(lambda d: dict(x=(d["x"] - 1) % 4))
X_FAR = perm(lambda d: dict(x=(d["x"] + 2) % 4))


def send(x, pairs):
    return lax.ppermute(x, AXES, pairs)


def vmem():
    return pl.BlockSpec(memory_space=pltpu.VMEM)


def smem():
    return pl.BlockSpec(memory_space=pltpu.SMEM)


def project_kernel(ids_ref, *refs):
    x_refs = refs[:8]
    gain_ref, w_ref, kv_ref, q_ref, out_ref, n_ref = refs[8:]
    tok = x_refs[0].shape[0]
    step = 128
    par = ids_ref[8]
    half = tok // 2
    lane = lax.broadcasted_iota(jnp.int32, (step, 128), 1)
    low = lane < HD

    def one(t, _):
        for part in range(2):
            rows = pl.ds(pl.multiple_of(part * half + t * step, step), step)
            parts = [x_ref[rows, :].astype(f32) for x_ref in x_refs]
            total = parts[0]
            for p in parts[1:]:
                total = total + p
            mean = jnp.sum(total, axis=1, keepdims=True) * (1.0 / D)
            sq = None
            for h in range(8):
                c = parts[h] - mean
                sq = c * c if sq is None else sq + c * c
            var = jnp.sum(sq, axis=1, keepdims=True) * (1.0 / D)
            inv = lax.rsqrt(var + 1e-06)
            for h in range(8):
                gain = gain_ref[ids_ref[h]]
                n_ref[ids_ref[h], part * step : (part + 1) * step] = ((parts[h] - mean) * inv * gain).astype(bf16)
        normed = jnp.concatenate([n_ref[h] for h in range(8)], axis=1)
        qk = jnp.dot(normed, jnp.concatenate([w_ref[0], w_ref[1]], axis=1), preferred_element_type=f32)
        v = jnp.dot(normed, w_ref[2], preferred_element_type=f32)
        k0, k1 = qk[:step, 128:], qk[step:, 128:]
        first = jnp.where(low, k0, pltpu.roll(k1, HD, 1))
        second = jnp.where(low, pltpu.roll(k0, HD, 1), k1)
        rows = pl.ds(pl.multiple_of(t * step, step), step)
        kv_ref[rows, :] = jnp.where(par > 0, second, first).astype(bf16)
        out_ref[rows, :] = jnp.where(par > 0, first, second).astype(bf16)
        for part in range(2):
            own = slice(part * step, (part + 1) * step)
            block = (part * (half // step) + t) * HD
            vt = v[own].T
            vkeep = jnp.where(par > 0, vt[HD:], vt[:HD])
            vgive = jnp.where(par > 0, vt[:HD], vt[HD:])
            to = pl.ds(pl.multiple_of(half + block, HD), HD)
            kv_ref[to, :] = vkeep.astype(bf16)
            out_ref[to, :] = vgive.astype(bf16)
            qt = (qk[own, :128] * QSCALE).T
            qkeep = jnp.where(par > 0, qt[HD:], qt[:HD])
            qgive = jnp.where(par > 0, qt[:HD], qt[HD:])
            q_ref[pl.ds(pl.multiple_of(block, HD), HD), :] = qkeep.astype(bf16)
            out_ref[pl.ds(pl.multiple_of(tok + block, HD), HD), :] = qgive.astype(bf16)
        return 0

    lax.fori_loop(0, half // step, one, 0)


def project(ids, blocks, gain, w):
    tok = blocks[0].shape[0]
    return pl.pallas_call(
        project_kernel,
        out_shape=(
            jax.ShapeDtypeStruct((tok, 128), bf16),
            jax.ShapeDtypeStruct((tok // 2, 128), bf16),
            jax.ShapeDtypeStruct((tok + tok // 2, 128), bf16),
        ),
        in_specs=[smem()] + [vmem()] * 10,
        out_specs=(vmem(), vmem(), vmem()),
        scratch_shapes=[pltpu.VMEM((8, 256, 128), bf16)],
        compiler_params=pltpu.CompilerParams(vmem_limit_bytes=40 << 20),
        name="project",
    )(ids, *blocks, gain, w)


def attend_kernel(*refs, npieces, nq, first, last, bq, bk, unroll, ahead):
    pieces = refs[:npieces]
    qs = refs[npieces : npieces + nq]
    rest = list(refs[npieces + nq :])
    if not first:
        acc_in, m_in = rest[:2]
        rest = rest[2:]
    if last:
        out_ref = rest[0]
        rest = rest[1:]
    acc_ref, m_ref, kvs, q2, s = rest
    ntiles = kvs.shape[0]
    per_tile = 1024 // bk
    nkb = ntiles * per_tile
    nqb = q2.shape[0]
    base = 0
    for piece in pieces:
        count = piece.shape[0] // 1024

        def load(i, _, piece=piece, base=base):
            for r in range(0, 1024, 256):
                kvs[base + i, r : r + 256] = piece[pl.ds(pl.multiple_of(i * 1024 + r, 256), 256), :]
            return 0

        lax.fori_loop(0, count, load, 0)
        base += count
    per = bq // 128
    zero = jnp.zeros((HD, bq), bf16)
    jb = 0
    for q in qs:
        for j in range(q.shape[0] // HD // per):
            blocks = [q[(j * per + b) * HD : (j * per + b + 1) * HD, :] for b in range(per)]
            block = jnp.concatenate(blocks, axis=1)
            q2[jb, 0, 0:HD] = block
            q2[jb, 0, HD:] = zero
            q2[jb, 1, 0:HD] = zero
            q2[jb, 1, HD:] = block
            jb += 1

    def scores(j, i):
        tile, sub = i // per_tile, i % per_tile
        k = kvs[tile, pl.ds(pl.multiple_of(sub * (bk // 2), 128), bk // 2)]
        return [jnp.dot(k, q2[j, e], preferred_element_type=f32) for e in range(2)]

    if first:
        for j in range(nqb):
            top = jnp.dot(kvs[0, 0:128], q2[j, 0], preferred_element_type=f32)
            m_ref[j] = jnp.max(top, axis=0, keepdims=True)
    else:
        m_ref[...] = m_in[...]

    def reset(j, _):
        acc_ref[j] = jnp.zeros(acc_ref.shape[1:], f32) if first else acc_in[j]
        return 0

    lax.fori_loop(0, nqb, reset, 0)

    steps = nqb * nkb

    units = [(c, g) for c in range(bk // 256) for g in range(bq // 256)]

    def unit(j, i, c, g):
        tile, sub = i // per_tile, i % per_tile
        half, row = (c * 256) // (bk // 2), (c * 256) % (bk // 2)
        k = kvs[tile, pl.ds(pl.multiple_of(sub * (bk // 2) + row, 128), 256)]
        return jnp.dot(k, q2[j, half, :, g * 256 : (g + 1) * 256], preferred_element_type=f32)

    def values(i, c):
        tile, sub = i // per_tile, i % per_tile
        half, row = (c * 256) // (bk // 2), (c * 256) % (bk // 2)
        at = [512 + (half * 4 + sub * (bk // 256) + row // 128 + b) * HD for b in range(2)]
        v = jnp.concatenate([kvs[tile, pl.ds(pl.multiple_of(x, HD), HD)] for x in at], axis=1)
        return jnp.concatenate([v, jnp.ones((16, 256), bf16)], axis=0)

    def trip(t):
        j, i = t // nkb, t % nkb
        u = jnp.where(t + 1 < steps, t + 1, 0)
        todo = [s[n] for n in range(ahead)] if ahead else []
        queue = [(j, i, c, g) for c, g in units]
        later = [(u // nkb, u % nkb, c, g) for c, g in units[:ahead]]
        order = queue[ahead:] + later
        accs = [acc_ref[j, :, g * 256 : (g + 1) * 256] for g in range(bq // 256)]
        tops = [m_ref[j, :, g * 256 : (g + 1) * 256] for g in range(bq // 256)]
        lead = max(ahead, 1)
        if not ahead:
            todo = [unit(*order.pop(0))]
        made = []
        for n, (jj, ii, c, g) in enumerate(queue):
            if order:
                nxt = unit(*order.pop(0))
                if len(order) < ahead and ahead:
                    made.append(nxt)
                else:
                    todo.append(nxt)
            p = jnp.exp2(todo[n] - tops[g]).astype(bf16)
            accs[g] = accs[g] + jnp.dot(values(i, c), p, preferred_element_type=f32)
        for n, v in enumerate(made):
            s[n] = v
        for g in range(bq // 256):
            acc_ref[j, :, g * 256 : (g + 1) * 256] = accs[g]

    def exact(j, _):
        def widen(i, top):
            for part in scores(j, i):
                top = jnp.maximum(top, jnp.max(part, axis=0, keepdims=True))
            return top

        if first:
            top = lax.fori_loop(0, nkb, widen, jnp.full((1, bq), -jnp.inf, f32))
            acc_ref[j] = jnp.zeros(acc_ref.shape[1:], f32)
        else:
            old = m_in[j]
            top = lax.fori_loop(0, nkb, widen, old)
            acc_ref[j] = acc_in[j] * jnp.exp2(old - top)
        m_ref[j] = top
        return 0

    def sweep(turn):
        @pl.when(turn > 0)
        def _():
            lax.fori_loop(0, nqb, exact, 0)

        for n in range(ahead):
            s[n] = unit(0, 0, *units[n])

        def some(h, _):
            for r in range(unroll):
                trip(unroll * h + r)
            return 0

        lax.fori_loop(0, steps // unroll, some, 0)
        den = acc_ref[:, HD : HD + 1, :]
        fine = jnp.min(jnp.where(den < CAP, 1.0, 0.0)) > 0.5
        return jnp.where(jnp.logical_or(turn > 0, fine), 2, 1)

    lax.while_loop(lambda turn: turn < 2, sweep, 0)

    if last:
        def finish(j, _):
            a = acc_ref[j]
            o = (a[0:HD] * (1.0 / a[HD : HD + 1])).astype(bf16)
            for b in range(per):
                out_ref[pl.ds(pl.multiple_of((j * per + b) * HD, HD), HD), :] = o[:, b * 128 : (b + 1) * 128]
            return 0

        lax.fori_loop(0, nqb, finish, 0)


def attend(name, pieces, qs, state=None, last=False, bq=512, bk=1024, unroll=8, ahead=4):
    nkeys = sum(p.shape[0] for p in pieces)
    nqueries = sum(q.shape[0] for q in qs) * 2
    nqb = nqueries // bq
    acc_shape = (nqb, HD + 16, bq)
    m_shape = (nqb, 1, bq)
    scratch = [
        pltpu.VMEM((nkeys // 1024, 1024, 128), bf16),
        pltpu.VMEM((nqb, 2, 128, bq), bf16),
        pltpu.VMEM((max(ahead, 1), 256, 256), f32),
    ]
    if last:
        out_shape = jax.ShapeDtypeStruct((nqueries // 2, 128), bf16)
        out_specs = vmem()
        scratch = [pltpu.VMEM(acc_shape, f32), pltpu.VMEM(m_shape, f32)] + scratch
    else:
        out_shape = (jax.ShapeDtypeStruct(acc_shape, f32), jax.ShapeDtypeStruct(m_shape, f32))
        out_specs = (vmem(), vmem())
    args = [*pieces, *qs] + ([] if state is None else list(state))
    flops = 4 * nkeys * nqueries * 128
    return pl.pallas_call(
        functools.partial(
            attend_kernel, npieces=len(pieces), nq=len(qs), first=state is None, last=last, bq=bq, bk=bk, unroll=unroll, ahead=ahead
        ),
        out_shape=out_shape,
        in_specs=[vmem()] * len(args),
        out_specs=out_specs,
        scratch_shapes=scratch,
        compiler_params=pltpu.CompilerParams(vmem_limit_bytes=48 << 20),
        cost_estimate=pl.CostEstimate(flops=flops, transcendentals=nkeys * nqueries, bytes_accessed=nkeys * 256),
        name=name,
    )(*args)


def mix_kernel(pos_ref, *refs):
    att_refs = refs[:4]
    own_ref, peer_ref = refs[4:6]
    out_refs = refs[6:10]
    w_ref = refs[10]
    for b in range(4):
        cols = pl.ds(pl.multiple_of((((pos_ref[0] + b) % 4) * 2 + pos_ref[1]) * 128, 128), 128)
        w_ref[0:128, b * 128 : (b + 1) * 128] = own_ref[:, cols]
        w_ref[128:256, b * 128 : (b + 1) * 128] = peer_ref[:, cols]

    def one(t, _):
        at = pl.ds(pl.multiple_of(t * HD, HD), HD)
        rows = jnp.concatenate([a[at, :] for a in att_refs], axis=0).T
        part = jnp.dot(rows, w_ref[...], preferred_element_type=f32).astype(bf16)
        to = pl.ds(pl.multiple_of(t * 128, 128), 128)
        for b in range(4):
            out_refs[b][to, :] = part[:, b * 128 : (b + 1) * 128]
        return 0

    lax.fori_loop(0, att_refs[0].shape[0] // HD, one, 0, unroll=2)


def mix(pos, att, own, peer):
    tok = att[0].shape[0] * 2
    return pl.pallas_call(
        mix_kernel,
        out_shape=[jax.ShapeDtypeStruct((tok, 128), bf16)] * 4,
        in_specs=[smem()] + [vmem()] * 6,
        out_specs=[vmem()] * 4,
        scratch_shapes=[pltpu.VMEM((256, 512), bf16)],
        compiler_params=pltpu.CompilerParams(vmem_limit_bytes=32 << 20),
        name="mix",
    )(pos, *att, own, peer)


def per_device(tokens, ln_gain, w_qkv, w_out, out_bias):
    rows = lax.axis_index("rows")
    heads = lax.axis_index("heads")
    yh = rows // 2
    x = heads // 2
    yl = heads % 2
    tok = tokens.shape[0]

    by_y = send(tokens, YL_SWAP)
    by_up = send(tokens, X_UP)
    by_down = send(tokens, X_DOWN)
    by_y, by_up, by_down, again = lax.optimization_barrier((by_y, by_up, by_down, tokens))
    y_up = send(by_up, YL_SWAP)
    y_down = send(by_down, YL_SWAP)
    by_far = send(again, X_FAR)
    y_far = send(by_y, X_FAR)
    blocks = (tokens, by_up, by_down, by_far, by_y, y_up, y_down, y_far)
    xs = jnp.stack([x, (x + 3) % 4, (x + 1) % 4, (x + 2) % 4])
    ids = jnp.concatenate([xs * 2 + yl, xs * 2 + 1 - yl, yh.reshape(1)]).astype(jnp.int32)

    kv, q, give = project(ids, blocks, ln_gain.reshape(8, 1, 128), w_qkv)
    got = send(give, YH_SWAP)
    q_far = got[tok:]
    near = jnp.concatenate([kv, got[:tok]], axis=0)
    near_other = send(near, CORE_SWAP)
    up = send(near, Z_UP)
    down = send(near, Z_DOWN)
    far = send(near, Z_FAR)
    qs = (q_far, q)
    state = attend("attend_near", (near, near_other), qs)
    up, down, state, w_send = lax.optimization_barrier((up, down, state, w_out))
    w_peer = send(w_send, YL_SWAP)
    up_other = send(up, CORE_SWAP)
    down_other = send(down, CORE_SWAP)
    state = attend("attend_ring", (up, down, up_other, down_other), qs, state)
    far, state = lax.optimization_barrier((far, state))
    far_other = send(far, CORE_SWAP)
    acc, m = state
    half = acc.shape[0] // 2
    att_far = attend("attend_last_far", (far, far_other), (q_far,), (acc[:half], m[:half]), last=True)
    back = send(att_far, YH_SWAP)
    att = attend("attend_last_near", (far, far_other), (q,), (acc[half:], m[half:]), last=True)
    peer_att = send(att, YL_SWAP)
    peer_back = send(back, YL_SWAP)
    att4 = [
        jnp.where(yh > 0, back, att),
        jnp.where(yh > 0, att, back),
        jnp.where(yh > 0, peer_back, peer_att),
        jnp.where(yh > 0, peer_att, peer_back),
    ]
    part = mix(jnp.stack([x, yl]).astype(jnp.int32), att4, w_out, w_peer)
    parts = [part[0], send(part[1], X_UP), send(part[2], X_FAR), send(part[3], X_DOWN)]
    summed = sum(p.astype(f32) for p in parts[1:]) + parts[0].astype(f32)
    return (tokens.astype(f32) + summed + out_bias).astype(bf16)


def solution(mesh):
    return jax.shard_map(
        per_device,
        mesh=mesh,
        in_specs=(
            P(("rows", "cols"), "heads"),
            P(),
            P(None, None, "heads"),
            P("heads", None),
            P("heads"),
        ),
        out_specs=P(("rows", "cols"), "heads"),
        check_vma=False,
    )
```

```python
import functools

import jax
import jax.numpy as jnp
from jax import lax
from jax.experimental import pallas as pl
from jax.experimental.pallas import tpu as pltpu
from jax.sharding import PartitionSpec as P


D = 1024
HD = 64
LOG2E = 1.4426950408889634
QSCALE = LOG2E / HD**0.5
CAP = 2.0**60
AXES = ("rows", "cols", "heads")
bf16 = jnp.bfloat16
f32 = jnp.float32


def perm(move):
    pairs = []
    for i in range(128):
        here = dict(x=(i % 8) // 2, yl=i % 2, z=(i // 8) % 4, yh=i // 64, c=(i // 32) % 2)
        to = {**here, **move(here)}
        pairs.append((i, ((to["yh"] * 2 + to["c"]) * 4 + to["z"]) * 8 + to["x"] * 2 + to["yl"]))
    return pairs


Z_UP = perm(lambda d: dict(z=(d["z"] + 1) % 4))
Z_DOWN = perm(lambda d: dict(z=(d["z"] - 1) % 4))
Z_FAR = perm(lambda d: dict(z=(d["z"] + 2) % 4))
YH_SWAP = perm(lambda d: dict(yh=1 - d["yh"]))
YL_SWAP = perm(lambda d: dict(yl=1 - d["yl"]))
CORE_SWAP = perm(lambda d: dict(c=1 - d["c"]))
X_UP = perm(lambda d: dict(x=(d["x"] + 1) % 4))
X_DOWN = perm(lambda d: dict(x=(d["x"] - 1) % 4))
X_FAR = perm(lambda d: dict(x=(d["x"] + 2) % 4))


def send(x, pairs):
    return lax.ppermute(x, AXES, pairs)


def vmem():
    return pl.BlockSpec(memory_space=pltpu.VMEM)


def hbm():
    return pl.BlockSpec(memory_space=pltpu.HBM)


def smem():
    return pl.BlockSpec(memory_space=pltpu.SMEM)


def project_kernel(ids_ref, own_hbm, *refs):
    x_refs = list(refs[:7])
    gain_ref, w_hbm, kv_ref, q_ref, out_ref, own_ref, w_ref, n_ref, sems = refs[7:]
    own_copy = pltpu.make_async_copy(own_hbm, own_ref, sems.at[0])
    w_copy = pltpu.make_async_copy(w_hbm, w_ref, sems.at[1])
    own_copy.start()
    w_copy.start()
    x_refs = [own_ref] + x_refs
    tok = own_ref.shape[0]
    step = 128
    par = ids_ref[8]
    half = tok // 2
    lane = lax.broadcasted_iota(jnp.int32, (step, 128), 1)
    low = lane < HD
    own_copy.wait()

    def norm(t, _):
        rows = pl.ds(pl.multiple_of(t * step, step), step)
        parts = [x_ref[rows, :].astype(f32) for x_ref in x_refs]
        total = parts[0]
        for p in parts[1:]:
            total = total + p
        mean = jnp.sum(total, axis=1, keepdims=True) * (1.0 / D)
        sq = None
        for h in range(8):
            c = parts[h] - mean
            sq = c * c if sq is None else sq + c * c
        var = jnp.sum(sq, axis=1, keepdims=True) * (1.0 / D)
        inv = lax.rsqrt(var + 1e-06)
        for h in range(8):
            gain = gain_ref[ids_ref[h]]
            n_ref[ids_ref[h], rows] = ((parts[h] - mean) * inv * gain).astype(bf16)
        return 0

    lax.fori_loop(0, tok // step, norm, 0, unroll=2)
    w_copy.wait()

    def one(t, _):
        at = [pl.ds(pl.multiple_of(part * half + t * step, step), step) for part in range(2)]
        normed = [jnp.concatenate([n_ref[h, a] for h in range(8)], axis=1) for a in at]
        normed = jnp.concatenate(normed, axis=0)
        qk = jnp.dot(normed, jnp.concatenate([w_ref[0], w_ref[1]], axis=1), preferred_element_type=f32)
        v = jnp.dot(normed, w_ref[2], preferred_element_type=f32)
        k0, k1 = qk[:step, 128:], qk[step:, 128:]
        first = jnp.where(low, k0, pltpu.roll(k1, HD, 1))
        second = jnp.where(low, pltpu.roll(k0, HD, 1), k1)
        rows = pl.ds(pl.multiple_of(t * step, step), step)
        kv_ref[rows, :] = jnp.where(par > 0, second, first).astype(bf16)
        out_ref[rows, :] = jnp.where(par > 0, first, second).astype(bf16)
        for part in range(2):
            own = slice(part * step, (part + 1) * step)
            block = (part * (half // step) + t) * HD
            vt = v[own].T
            vkeep = jnp.where(par > 0, vt[HD:], vt[:HD])
            vgive = jnp.where(par > 0, vt[:HD], vt[HD:])
            to = pl.ds(pl.multiple_of(half + block, HD), HD)
            kv_ref[to, :] = vkeep.astype(bf16)
            out_ref[to, :] = vgive.astype(bf16)
            qt = (qk[own, :128] * QSCALE).T
            qkeep = jnp.where(par > 0, qt[HD:], qt[:HD])
            qgive = jnp.where(par > 0, qt[:HD], qt[HD:])
            q_ref[pl.ds(pl.multiple_of(block, HD), HD), :] = qkeep.astype(bf16)
            out_ref[pl.ds(pl.multiple_of(tok + block, HD), HD), :] = qgive.astype(bf16)
        return 0

    lax.fori_loop(0, half // step, one, 0, unroll=2)


def project(ids, blocks, gain, w):
    tok = blocks[0].shape[0]
    return pl.pallas_call(
        project_kernel,
        out_shape=(
            jax.ShapeDtypeStruct((tok, 128), bf16),
            jax.ShapeDtypeStruct((tok // 2, 128), bf16),
            jax.ShapeDtypeStruct((tok + tok // 2, 128), bf16),
        ),
        in_specs=[smem(), hbm()] + [vmem()] * 8 + [hbm()],
        out_specs=(vmem(), vmem(), vmem()),
        scratch_shapes=[
            pltpu.VMEM((tok, 128), bf16),
            pltpu.VMEM(w.shape, bf16),
            pltpu.VMEM((8, tok, 128), bf16),
            pltpu.SemaphoreType.DMA((2,)),
        ],
        compiler_params=pltpu.CompilerParams(vmem_limit_bytes=12 << 20),
        name="project",
    )(ids, *blocks, gain, w)


def attend_kernel(*refs, npieces, windows, offset, first, outs, bq, bk, unroll, ahead):
    pieces = refs[:npieces]
    qs = refs[npieces : npieces + len(windows)]
    rest = list(refs[npieces + len(windows) :])
    if not first:
        acc_in, m_in = rest[:2]
        rest = rest[2:]
    out_refs = rest[:outs]
    rest = rest[outs:]
    acc_ref, m_ref, kvs, q2, s = rest
    ntiles = kvs.shape[0]
    per_tile = 1024 // bk
    nkb = ntiles * per_tile
    nqb = q2.shape[0]
    base = 0
    for piece in pieces:
        count = piece.shape[0] // 1024

        def load(i, _, piece=piece, base=base):
            for r in range(0, 1024, 256):
                kvs[base + i, r : r + 256] = piece[pl.ds(pl.multiple_of(i * 1024 + r, 256), 256), :]
            return 0

        lax.fori_loop(0, count, load, 0)
        base += count
    per = bq // 128
    zero = jnp.zeros((HD, bq), bf16)
    jb = 0
    for q, (start, count) in zip(qs, windows):
        for j in range(count // HD // per):
            blocks = [q[start + (j * per + b) * HD : start + (j * per + b + 1) * HD, :] for b in range(per)]
            block = jnp.concatenate(blocks, axis=1)
            q2[jb, 0, 0:HD] = block
            q2[jb, 0, HD:] = zero
            q2[jb, 1, 0:HD] = zero
            q2[jb, 1, HD:] = block
            jb += 1

    def scores(j, i):
        tile, sub = i // per_tile, i % per_tile
        k = kvs[tile, pl.ds(pl.multiple_of(sub * (bk // 2), 128), bk // 2)]
        return [jnp.dot(k, q2[j, e], preferred_element_type=f32) for e in range(2)]

    if first:
        for j in range(nqb):
            top = jnp.dot(kvs[0, 0:128], q2[j, 0], preferred_element_type=f32)
            m_ref[j] = jnp.max(top, axis=0, keepdims=True)
    else:
        for j in range(nqb):
            m_ref[j] = m_in[offset + j]

    def reset(j, _):
        acc_ref[j] = jnp.zeros(acc_ref.shape[1:], f32) if first else acc_in[offset + j]
        return 0

    lax.fori_loop(0, nqb, reset, 0)

    steps = nqb * nkb

    units = [(c, g) for c in range(bk // 256) for g in range(bq // 256)]

    def unit(j, i, c, g):
        tile, sub = i // per_tile, i % per_tile
        half, row = (c * 256) // (bk // 2), (c * 256) % (bk // 2)
        k = kvs[tile, pl.ds(pl.multiple_of(sub * (bk // 2) + row, 128), 256)]
        return jnp.dot(k, q2[j, half, :, g * 256 : (g + 1) * 256], preferred_element_type=f32)

    def values(i, c):
        tile, sub = i // per_tile, i % per_tile
        half, row = (c * 256) // (bk // 2), (c * 256) % (bk // 2)
        at = [512 + (half * 4 + sub * (bk // 256) + row // 128 + b) * HD for b in range(2)]
        v = jnp.concatenate([kvs[tile, pl.ds(pl.multiple_of(x, HD), HD)] for x in at], axis=1)
        return jnp.concatenate([v, jnp.ones((16, 256), bf16)], axis=0)

    def trip(t):
        j, i = t // nkb, t % nkb
        u = jnp.where(t + 1 < steps, t + 1, 0)
        todo = [s[n] for n in range(ahead)] if ahead else []
        queue = [(j, i, c, g) for c, g in units]
        later = [(u // nkb, u % nkb, c, g) for c, g in units[:ahead]]
        order = queue[ahead:] + later
        accs = [acc_ref[j, :, g * 256 : (g + 1) * 256] for g in range(bq // 256)]
        tops = [m_ref[j, :, g * 256 : (g + 1) * 256] for g in range(bq // 256)]
        if not ahead:
            todo = [unit(*order.pop(0))]
        made = []
        for n, (jj, ii, c, g) in enumerate(queue):
            if order:
                nxt = unit(*order.pop(0))
                if len(order) < ahead and ahead:
                    made.append(nxt)
                else:
                    todo.append(nxt)
            p = jnp.exp2(todo[n] - tops[g]).astype(bf16)
            accs[g] = accs[g] + jnp.dot(values(i, c), p, preferred_element_type=f32)
        for n, v in enumerate(made):
            s[n] = v
        for g in range(bq // 256):
            acc_ref[j, :, g * 256 : (g + 1) * 256] = accs[g]

    def exact(j, _):
        def widen(i, top):
            for part in scores(j, i):
                top = jnp.maximum(top, jnp.max(part, axis=0, keepdims=True))
            return top

        if first:
            top = lax.fori_loop(0, nkb, widen, jnp.full((1, bq), -jnp.inf, f32))
            acc_ref[j] = jnp.zeros(acc_ref.shape[1:], f32)
        else:
            old = m_in[offset + j]
            top = lax.fori_loop(0, nkb, widen, old)
            acc_ref[j] = acc_in[offset + j] * jnp.exp2(old - top)
        m_ref[j] = top
        return 0

    def sweep(turn):
        @pl.when(turn > 0)
        def _():
            lax.fori_loop(0, nqb, exact, 0)

        for n in range(ahead):
            s[n] = unit(0, 0, *units[n])

        def some(h, _):
            for r in range(unroll):
                trip(unroll * h + r)
            return 0

        lax.fori_loop(0, steps // unroll, some, 0)
        den = acc_ref[:, HD : HD + 1, :]
        fine = jnp.min(jnp.where(den < CAP, 1.0, 0.0)) > 0.5
        return jnp.where(jnp.logical_or(turn > 0, fine), 2, 1)

    lax.while_loop(lambda turn: turn < 2, sweep, 0)

    for n, out_ref in enumerate(out_refs):
        for j in range(nqb // outs):
            a = acc_ref[n * (nqb // outs) + j]
            o = (a[0:HD] * (1.0 / a[HD : HD + 1])).astype(bf16)
            for b in range(per):
                out_ref[(j * per + b) * HD : (j * per + b + 1) * HD, :] = o[:, b * 128 : (b + 1) * 128]


def attend(pieces, qs, state=None, offset=0, outs=0, bq=512, bk=1024, unroll=8, ahead=4):
    windows = tuple(w for q, w in qs)
    nkeys = sum(p.shape[0] for p in pieces)
    nqueries = sum(count for start, count in windows) * 2
    nqb = nqueries // bq
    acc_shape = (nqb, HD + 16, bq)
    m_shape = (nqb, 1, bq)
    scratch = [
        pltpu.VMEM((nkeys // 1024, 1024, 128), bf16),
        pltpu.VMEM((nqb, 2, 128, bq), bf16),
        pltpu.VMEM((max(ahead, 1), 256, 256), f32),
    ]
    if outs:
        out_shape = [jax.ShapeDtypeStruct((nqueries // 2 // outs, 128), bf16)] * outs
        out_specs = [vmem()] * outs
        scratch = [pltpu.VMEM(acc_shape, f32), pltpu.VMEM(m_shape, f32)] + scratch
    else:
        out_shape = (jax.ShapeDtypeStruct(acc_shape, f32), jax.ShapeDtypeStruct(m_shape, f32))
        out_specs = (vmem(), vmem())
    args = [*pieces, *(q for q, w in qs)] + ([] if state is None else list(state))
    flops = 4 * nkeys * nqueries * 128
    return pl.pallas_call(
        functools.partial(
            attend_kernel, npieces=len(pieces), windows=windows, offset=offset, first=state is None, outs=outs, bq=bq, bk=bk, unroll=unroll, ahead=ahead
        ),
        out_shape=out_shape,
        in_specs=[vmem()] * len(args),
        out_specs=out_specs,
        scratch_shapes=scratch,
        compiler_params=pltpu.CompilerParams(vmem_limit_bytes=16 << 20),
        cost_estimate=pl.CostEstimate(flops=flops, transcendentals=nkeys * nqueries, bytes_accessed=nkeys * 256),
    )(*args)


def mix_kernel(pos_ref, *refs, part):
    kept, back, peer_kept, peer_back = refs[:4]
    swap = pos_ref[2] > 0
    own_ref, peer_ref = refs[4:6]
    out_refs = refs[6:10]
    w_ref = refs[10]
    for b in range(4):
        cols = pl.ds(pl.multiple_of((((pos_ref[0] + b) % 4) * 2 + pos_ref[1]) * 128, 128), 128)
        w_ref[0:128, b * 128 : (b + 1) * 128] = own_ref[:, cols]
        w_ref[128:256, b * 128 : (b + 1) * 128] = peer_ref[:, cols]

    count = kept.shape[0] // HD

    def one(t, _):
        at = pl.ds(pl.multiple_of(t * HD, HD), HD)
        also = pl.ds(pl.multiple_of((part * count + t) * HD, HD), HD)
        cols = []
        for mine, other in ((kept, back), (peer_kept, peer_back)):
            a, b = mine[at, :], other[also, :]
            cols += [jnp.where(swap, b, a), jnp.where(swap, a, b)]
        rows = jnp.concatenate(cols, axis=0).T
        out = jnp.dot(rows, w_ref[...], preferred_element_type=f32).astype(bf16)
        to = pl.ds(pl.multiple_of(t * 128, 128), 128)
        for b in range(4):
            out_refs[b][to, :] = out[:, b * 128 : (b + 1) * 128]
        return 0

    lax.fori_loop(0, count, one, 0, unroll=2)


def mix(pos, att, own, peer, part):
    tok = att[0].shape[0] * 2
    return pl.pallas_call(
        functools.partial(mix_kernel, part=part),
        out_shape=[jax.ShapeDtypeStruct((tok, 128), bf16)] * 4,
        in_specs=[smem()] + [vmem()] * 6,
        out_specs=[vmem()] * 4,
        scratch_shapes=[pltpu.VMEM((256, 512), bf16)],
        compiler_params=pltpu.CompilerParams(vmem_limit_bytes=6 << 20),
    )(pos, *att, own, peer)


def per_device(tokens, ln_gain, w_qkv, w_out, out_bias):
    rows = lax.axis_index("rows")
    heads = lax.axis_index("heads")
    yh = rows // 2
    x = heads // 2
    yl = heads % 2
    tok = tokens.shape[0]

    by_y = send(tokens, YL_SWAP)
    by_up = send(tokens, X_UP)
    by_down = send(tokens, X_DOWN)
    y_far = send(by_y, X_FAR)
    y_up = send(by_up, YL_SWAP)
    y_down = send(by_down, YL_SWAP)
    by_far = send(tokens, X_FAR)
    blocks = (tokens, by_up, by_down, by_far, by_y, y_up, y_down, y_far)
    xs = jnp.stack([x, (x + 3) % 4, (x + 1) % 4, (x + 2) % 4])
    ids = jnp.concatenate([xs * 2 + yl, xs * 2 + 1 - yl, yh.reshape(1)]).astype(jnp.int32)

    kv, q, give = project(ids, blocks, ln_gain.reshape(8, 1, 128), pltpu.with_memory_space_constraint(w_qkv, pltpu.HBM))
    got = send(give, YH_SWAP)
    k_other = send(kv, CORE_SWAP)
    k_up = send(kv, Z_UP)
    k_down = send(kv, Z_DOWN)
    kf = got[:tok]
    f_other = send(kf, CORE_SWAP)
    f_up = send(kf, Z_UP)
    f_down = send(kf, Z_DOWN)
    qs = ((got, (tok, tok // 2)), (q, (0, tok // 2)))
    state = attend((kv, kf, k_other, f_other), qs)
    k_up, k_down, f_up, f_down, w_send, state = lax.optimization_barrier((k_up, k_down, f_up, f_down, w_out, state))
    k_far = send(k_up, Z_UP)
    f_far = send(f_down, Z_DOWN)
    ring = (k_up, k_down, f_up, f_down)
    ring = ring + tuple(send(p, CORE_SWAP) for p in ring)
    w_peer = send(w_send, YL_SWAP)
    state = attend(ring, qs, state)
    ends = (k_far, f_far, send(k_far, CORE_SWAP), send(f_far, CORE_SWAP))
    (att_far,) = attend(ends, qs[:1], state, outs=1)
    back = send(att_far, YH_SWAP)
    q_own, att_far = lax.optimization_barrier((q, att_far))
    att = attend(ends, ((q_own, (0, tok // 2)),), state, offset=2, outs=2)
    peer = [send(att[0], YL_SWAP), send(att[1], YL_SWAP)]
    peer_back = send(back, YL_SWAP)
    pos = jnp.stack([x, yl, yh]).astype(jnp.int32)
    parts = []
    for n in range(2):
        part = mix(pos, (att[n], back, peer[n], peer_back), w_out, w_peer, n)
        here = [part[0]]
        for b, pairs in ((1, X_UP), (2, X_FAR), (3, X_DOWN)):
            here.append(send(part[b], pairs))
        parts.append(here)
    summed = sum(jnp.concatenate([parts[0][b], parts[1][b]], axis=0).astype(f32) for b in range(4))
    return (tokens.astype(f32) + summed + out_bias).astype(bf16)


def solution(mesh):
    return jax.shard_map(
        per_device,
        mesh=mesh,
        in_specs=(
            P(("rows", "cols"), "heads"),
            P(),
            P(None, None, "heads"),
            P("heads", None),
            P("heads"),
        ),
        out_specs=P(("rows", "cols"), "heads"),
        check_vma=False,
    )
```

```python
import functools

import jax
import jax.numpy as jnp
from jax import lax
from jax.experimental import pallas as pl
from jax.experimental.pallas import tpu as pltpu
from jax.sharding import PartitionSpec as P


D = 1024
HD = 64
LOG2E = 1.4426950408889634
QSCALE = LOG2E / HD**0.5
CAP = 2.0**60
AXES = ("rows", "cols", "heads")
bf16 = jnp.bfloat16
f32 = jnp.float32


def perm(move):
    pairs = []
    for i in range(128):
        here = dict(x=(i % 8) // 2, yl=i % 2, z=(i // 8) % 4, yh=i // 64, c=(i // 32) % 2)
        to = {**here, **move(here)}
        pairs.append((i, ((to["yh"] * 2 + to["c"]) * 4 + to["z"]) * 8 + to["x"] * 2 + to["yl"]))
    return pairs


Z_UP = perm(lambda d: dict(z=(d["z"] + 1) % 4))
Z_DOWN = perm(lambda d: dict(z=(d["z"] - 1) % 4))
Z_FAR = perm(lambda d: dict(z=(d["z"] + 2) % 4))
YH_SWAP = perm(lambda d: dict(yh=1 - d["yh"]))
YL_SWAP = perm(lambda d: dict(yl=1 - d["yl"]))
CORE_SWAP = perm(lambda d: dict(c=1 - d["c"]))
X_UP = perm(lambda d: dict(x=(d["x"] + 1) % 4))
X_DOWN = perm(lambda d: dict(x=(d["x"] - 1) % 4))
X_FAR = perm(lambda d: dict(x=(d["x"] + 2) % 4))


def send(x, pairs):
    return lax.ppermute(x, AXES, pairs)


def vmem():
    return pl.BlockSpec(memory_space=pltpu.VMEM)


def hbm():
    return pl.BlockSpec(memory_space=pltpu.HBM)


def smem():
    return pl.BlockSpec(memory_space=pltpu.SMEM)


def project_kernel(ids_ref, *refs):
    x_refs = refs[:8]
    gain_ref, w_ref, kv_ref, q_ref, out_ref, n_even, n_odd = refs[8:]
    tok = x_refs[0].shape[0]
    step = 128
    half = tok // 2
    par = ids_ref[8]
    lane = lax.broadcasted_iota(jnp.int32, (step, 128), 1)
    low = lane < HD

    def norm(t, n_ref):
        for part in range(2):
            for r in range(0, step, 32):
                rows = slice(part * half + t * step + r, part * half + t * step + r + 32)
                parts = [x_ref[rows, :].astype(f32) for x_ref in x_refs]
                total = parts[0]
                for p in parts[1:]:
                    total = total + p
                mean = jnp.sum(total, axis=1, keepdims=True) * (1.0 / D)
                cs = [p - mean for p in parts]
                sq = cs[0] * cs[0]
                for c in cs[1:]:
                    sq = sq + c * c
                var = jnp.sum(sq, axis=1, keepdims=True) * (1.0 / D)
                inv = lax.rsqrt(var + 1e-06)
                for h in range(8):
                    to = slice(part * step + r, part * step + r + 32)
                    n_ref[ids_ref[h], to] = (cs[h] * inv * gain_ref[ids_ref[h]]).astype(bf16)

    def one(t, n_ref):
        normed = jnp.concatenate([n_ref[h] for h in range(8)], axis=1)
        qk = jnp.dot(normed, jnp.concatenate([w_ref[0], w_ref[1]], axis=1), preferred_element_type=f32)
        v = jnp.dot(normed, w_ref[2], preferred_element_type=f32)
        k0, k1 = qk[:step, 128:], qk[step:, 128:]
        first = jnp.where(low, k0, pltpu.roll(k1, HD, 1))
        second = jnp.where(low, pltpu.roll(k0, HD, 1), k1)
        rows = slice(t * step, (t + 1) * step)
        kv_ref[rows, :] = jnp.where(par > 0, second, first).astype(bf16)
        out_ref[rows, :] = jnp.where(par > 0, first, second).astype(bf16)
        for part in range(2):
            own = slice(part * step, (part + 1) * step)
            block = (part * (half // step) + t) * HD
            vt = v[own].T
            vkeep = jnp.where(par > 0, vt[HD:], vt[:HD])
            vgive = jnp.where(par > 0, vt[:HD], vt[HD:])
            to = slice(half + block, half + block + HD)
            kv_ref[to, :] = vkeep.astype(bf16)
            out_ref[to, :] = vgive.astype(bf16)
            qt = (qk[own, :128] * QSCALE).T
            qkeep = jnp.where(par > 0, qt[HD:], qt[:HD])
            qgive = jnp.where(par > 0, qt[:HD], qt[HD:])
            q_ref[block : block + HD, :] = qkeep.astype(bf16)
            out_ref[tok + block : tok + block + HD, :] = qgive.astype(bf16)

    bufs = (n_even, n_odd)
    trips = half // step
    norm(0, bufs[0])
    for t in range(trips):
        if t + 1 < trips:
            norm(t + 1, bufs[(t + 1) % 2])
        one(t, bufs[t % 2])


def stage_kernel(x_ref, w_ref, xo_ref, wo_ref, sems):
    copies = [
        pltpu.make_async_copy(x_ref, xo_ref, sems.at[0]),
        pltpu.make_async_copy(w_ref, wo_ref, sems.at[1]),
    ]
    for c in copies:
        c.start()
    for c in copies:
        c.wait()


def stage(x, w):
    x, w = (pltpu.with_memory_space_constraint(a, pltpu.HBM) for a in (x, w))
    return pl.pallas_call(
        stage_kernel,
        out_shape=(jax.ShapeDtypeStruct(x.shape, x.dtype), jax.ShapeDtypeStruct(w.shape, w.dtype)),
        in_specs=[hbm(), hbm()],
        out_specs=(vmem(), vmem()),
        scratch_shapes=[pltpu.SemaphoreType.DMA((2,))],
        compiler_params=pltpu.CompilerParams(vmem_limit_bytes=2 << 20),
        name="stage",
    )(x, w)


def project(ids, blocks, gain, w):
    tok = blocks[0].shape[0]
    return pl.pallas_call(
        project_kernel,
        out_shape=(
            jax.ShapeDtypeStruct((tok, 128), bf16),
            jax.ShapeDtypeStruct((tok // 2, 128), bf16),
            jax.ShapeDtypeStruct((tok + tok // 2, 128), bf16),
        ),
        in_specs=[smem()] + [vmem()] * 10,
        out_specs=(vmem(), vmem(), vmem()),
        scratch_shapes=[
            pltpu.VMEM((8, 256, 128), bf16),
            pltpu.VMEM((8, 256, 128), bf16),
        ],
        compiler_params=pltpu.CompilerParams(vmem_limit_bytes=12 << 20),
        name="project",
    )(ids, *blocks, gain, w)


def attend_kernel(*refs, npieces, windows, offset, first, outs, bq, bk, unroll, ahead):
    pieces = refs[:npieces]
    qs = refs[npieces : npieces + len(windows)]
    rest = list(refs[npieces + len(windows) :])
    if not first:
        acc_in, m_in = rest[:2]
        rest = rest[2:]
    out_refs = rest[:outs]
    rest = rest[outs:]
    acc_ref, m_ref, kvs, q2, s = rest
    ntiles = kvs.shape[0]
    per_tile = 1024 // bk
    nkb = ntiles * per_tile
    nqb = q2.shape[0]
    base = 0
    for piece in pieces:
        count = piece.shape[0] // 1024

        def load(i, _, piece=piece, base=base):
            for r in range(0, 1024, 256):
                kvs[base + i, r : r + 256] = piece[pl.ds(pl.multiple_of(i * 1024 + r, 256), 256), :]
            return 0

        lax.fori_loop(0, count, load, 0)
        base += count
    per = bq // 128
    zero = jnp.zeros((HD, bq), bf16)
    jb = 0
    for q, (start, count) in zip(qs, windows):
        for j in range(count // HD // per):
            blocks = [q[start + (j * per + b) * HD : start + (j * per + b + 1) * HD, :] for b in range(per)]
            block = jnp.concatenate(blocks, axis=1)
            q2[jb, 0, 0:HD] = block
            q2[jb, 0, HD:] = zero
            q2[jb, 1, 0:HD] = zero
            q2[jb, 1, HD:] = block
            jb += 1

    def scores(j, i):
        tile, sub = i // per_tile, i % per_tile
        k = kvs[tile, pl.ds(pl.multiple_of(sub * (bk // 2), 128), bk // 2)]
        return [jnp.dot(k, q2[j, e], preferred_element_type=f32) for e in range(2)]

    if first:
        for j in range(nqb):
            top = jnp.dot(kvs[0, 0:128], q2[j, 0], preferred_element_type=f32)
            m_ref[j] = jnp.max(top, axis=0, keepdims=True)
    else:
        for j in range(nqb):
            m_ref[j] = m_in[offset + j]

    def reset(j, _):
        acc_ref[j] = jnp.zeros(acc_ref.shape[1:], f32) if first else acc_in[offset + j]
        return 0

    lax.fori_loop(0, nqb, reset, 0)

    steps = nqb * nkb

    units = [(c, g) for c in range(bk // 256) for g in range(bq // 256)]

    def unit(j, i, c, g):
        tile, sub = i // per_tile, i % per_tile
        half, row = (c * 256) // (bk // 2), (c * 256) % (bk // 2)
        k = kvs[tile, pl.ds(pl.multiple_of(sub * (bk // 2) + row, 128), 256)]
        return jnp.dot(k, q2[j, half, :, g * 256 : (g + 1) * 256], preferred_element_type=f32)

    def values(i, c):
        tile, sub = i // per_tile, i % per_tile
        half, row = (c * 256) // (bk // 2), (c * 256) % (bk // 2)
        at = [512 + (half * 4 + sub * (bk // 256) + row // 128 + b) * HD for b in range(2)]
        return jnp.concatenate([kvs[tile, pl.ds(pl.multiple_of(x, HD), HD)] for x in at], axis=1)

    def trip(t):
        j, i = t // nkb, t % nkb
        u = jnp.where(t + 1 < steps, t + 1, 0)
        todo = [s[n] for n in range(ahead)] if ahead else []
        queue = [(j, i, c, g) for c, g in units]
        later = [(u // nkb, u % nkb, c, g) for c, g in units[:ahead]]
        order = queue[ahead:] + later
        accs = [acc_ref[j, :HD, g * 256 : (g + 1) * 256] for g in range(bq // 256)]
        dens = [acc_ref[j, HD:, g * 256 : (g + 1) * 256] for g in range(bq // 256)]
        tops = [m_ref[j, :, g * 256 : (g + 1) * 256] for g in range(bq // 256)]
        if not ahead:
            todo = [unit(*order.pop(0))]
        made = []
        for n, (jj, ii, c, g) in enumerate(queue):
            if order:
                nxt = unit(*order.pop(0))
                if len(order) < ahead and ahead:
                    made.append(nxt)
                else:
                    todo.append(nxt)
            p = jnp.exp2(todo[n] - tops[g])
            dens[g] = dens[g] + jnp.sum(p.reshape(32, 8, 256), axis=0)
            accs[g] = accs[g] + jnp.dot(values(i, c), p.astype(bf16), preferred_element_type=f32)
        for n, v in enumerate(made):
            s[n] = v
        for g in range(bq // 256):
            acc_ref[j, :HD, g * 256 : (g + 1) * 256] = accs[g]
            acc_ref[j, HD:, g * 256 : (g + 1) * 256] = dens[g]

    def exact(j, _):
        def widen(i, top):
            for part in scores(j, i):
                top = jnp.maximum(top, jnp.max(part, axis=0, keepdims=True))
            return top

        if first:
            top = lax.fori_loop(0, nkb, widen, jnp.full((1, bq), -jnp.inf, f32))
            acc_ref[j] = jnp.zeros(acc_ref.shape[1:], f32)
        else:
            old = m_in[offset + j]
            top = lax.fori_loop(0, nkb, widen, old)
            acc_ref[j] = acc_in[offset + j] * jnp.exp2(old - top)
        m_ref[j] = top
        return 0

    def sweep(turn):
        @pl.when(turn > 0)
        def _():
            lax.fori_loop(0, nqb, exact, 0)

        for n in range(ahead):
            s[n] = unit(0, 0, *units[n])

        def some(h, _):
            for r in range(unroll):
                trip(unroll * h + r)
            return 0

        lax.fori_loop(0, steps // unroll, some, 0)
        den = acc_ref[:, HD:, :]
        fine = jnp.min(jnp.where(den < CAP, 1.0, 0.0)) > 0.5
        return jnp.where(jnp.logical_or(turn > 0, fine), 2, 1)

    lax.while_loop(lambda turn: turn < 2, sweep, 0)

    for n, out_ref in enumerate(out_refs):
        for j in range(nqb // outs):
            a = acc_ref[n * (nqb // outs) + j]
            o = (a[0:HD] * (1.0 / jnp.sum(a[HD:], axis=0, keepdims=True))).astype(bf16)
            for b in range(per):
                out_ref[(j * per + b) * HD : (j * per + b + 1) * HD, :] = o[:, b * 128 : (b + 1) * 128]


def attend(pieces, qs, state=None, offset=0, outs=0, bq=512, bk=1024, unroll=8, ahead=4):
    windows = tuple(w for q, w in qs)
    nkeys = sum(p.shape[0] for p in pieces)
    nqueries = sum(count for start, count in windows) * 2
    nqb = nqueries // bq
    acc_shape = (nqb, HD + 8, bq)
    m_shape = (nqb, 1, bq)
    scratch = [
        pltpu.VMEM((nkeys // 1024, 1024, 128), bf16),
        pltpu.VMEM((nqb, 2, 128, bq), bf16),
        pltpu.VMEM((max(ahead, 1), 256, 256), f32),
    ]
    if outs:
        out_shape = [jax.ShapeDtypeStruct((nqueries // 2 // outs, 128), bf16)] * outs
        out_specs = [vmem()] * outs
        scratch = [pltpu.VMEM(acc_shape, f32), pltpu.VMEM(m_shape, f32)] + scratch
    else:
        out_shape = (jax.ShapeDtypeStruct(acc_shape, f32), jax.ShapeDtypeStruct(m_shape, f32))
        out_specs = (vmem(), vmem())
    args = [*pieces, *(q for q, w in qs)] + ([] if state is None else list(state))
    flops = 4 * nkeys * nqueries * 128
    return pl.pallas_call(
        functools.partial(
            attend_kernel, npieces=len(pieces), windows=windows, offset=offset, first=state is None, outs=outs, bq=bq, bk=bk, unroll=unroll, ahead=ahead
        ),
        out_shape=out_shape,
        in_specs=[vmem()] * len(args),
        out_specs=out_specs,
        scratch_shapes=scratch,
        compiler_params=pltpu.CompilerParams(vmem_limit_bytes=16 << 20),
        cost_estimate=pl.CostEstimate(flops=flops, transcendentals=nkeys * nqueries, bytes_accessed=nkeys * 256),
    )(*args)


def mix_kernel(pos_ref, *refs, part):
    kept, back, peer_kept, peer_back = refs[:4]
    swap = pos_ref[2] > 0
    own_ref, peer_ref, x_ref, bias_ref = refs[4:8]
    base_ref = refs[8]
    out_refs = refs[9:12]
    w_ref = refs[12]
    for b in range(4):
        cols = pl.ds(pl.multiple_of((((pos_ref[0] + b) % 4) * 2 + pos_ref[1]) * 128, 128), 128)
        w_ref[0:128, b * 128 : (b + 1) * 128] = own_ref[:, cols]
        w_ref[128:256, b * 128 : (b + 1) * 128] = peer_ref[:, cols]

    count = kept.shape[0] // HD

    def one(t, _):
        at = pl.ds(pl.multiple_of(t * HD, HD), HD)
        also = pl.ds(pl.multiple_of((part * count + t) * HD, HD), HD)
        cols = []
        for mine, other in ((kept, back), (peer_kept, peer_back)):
            a, b = mine[at, :], other[also, :]
            cols += [jnp.where(swap, b, a), jnp.where(swap, a, b)]
        rows = jnp.concatenate(cols, axis=0).T
        out = jnp.dot(rows, w_ref[...], preferred_element_type=f32)
        to = pl.ds(pl.multiple_of(t * 128, 128), 128)
        come = pl.ds(pl.multiple_of((part * count + t) * 128, 128), 128)
        base_ref[to, :] = out[:, :128] + x_ref[come, :].astype(f32) + bias_ref[...]
        for b in range(3):
            out_refs[b][to, :] = out[:, (b + 1) * 128 : (b + 2) * 128].astype(bf16)
        return 0

    lax.fori_loop(0, count, one, 0, unroll=2)


def mix(pos, att, own, peer, x, bias, part):
    tok = att[0].shape[0] * 2
    return pl.pallas_call(
        functools.partial(mix_kernel, part=part),
        out_shape=[jax.ShapeDtypeStruct((tok, 128), f32)] + [jax.ShapeDtypeStruct((tok, 128), bf16)] * 3,
        in_specs=[smem()] + [vmem()] * 8,
        out_specs=[vmem()] * 4,
        scratch_shapes=[pltpu.VMEM((256, 512), bf16)],
        compiler_params=pltpu.CompilerParams(vmem_limit_bytes=6 << 20),
    )(pos, *att, own, peer, x, bias)


def per_device(tokens, ln_gain, w_qkv, w_out, out_bias):
    rows = lax.axis_index("rows")
    heads = lax.axis_index("heads")
    yh = rows // 2
    x = heads // 2
    yl = heads % 2
    tok = tokens.shape[0]

    by_y = send(tokens, YL_SWAP)
    by_up = send(tokens, X_UP)
    by_down = send(tokens, X_DOWN)
    by_far = send(tokens, X_FAR)
    y_far = send(by_y, X_FAR)
    y_up = send(by_up, YL_SWAP)
    y_down = send(by_down, YL_SWAP)
    held, w_held = stage(tokens, w_qkv)
    blocks = (held, by_up, by_down, by_far, by_y, y_up, y_down, y_far)
    xs = jnp.stack([x, (x + 3) % 4, (x + 1) % 4, (x + 2) % 4])
    ids = jnp.concatenate([xs * 2 + yl, xs * 2 + 1 - yl, yh.reshape(1)]).astype(jnp.int32)

    kv, q, give = project(ids, blocks, ln_gain.reshape(8, 1, 128), w_held)
    got = send(give, YH_SWAP)
    k_other = send(kv, CORE_SWAP)
    k_up = send(kv, Z_UP)
    k_down = send(kv, Z_DOWN)
    kf = got[:tok]
    f_other = send(kf, CORE_SWAP)
    f_up = send(kf, Z_UP)
    f_down = send(kf, Z_DOWN)
    qs = ((got, (tok, tok // 2)), (q, (0, tok // 2)))
    state = attend((kv, kf, k_other, f_other), qs)
    k_up, k_down, f_up, f_down, w_send, state = lax.optimization_barrier((k_up, k_down, f_up, f_down, w_out, state))
    k_far = send(k_up, Z_UP)
    f_far = send(f_down, Z_DOWN)
    ring = (k_up, k_down, f_up, f_down)
    ring = ring + tuple(send(p, CORE_SWAP) for p in ring)
    w_peer = send(w_send, YL_SWAP)
    state = attend(ring, qs, state)
    ends = (k_far, f_far, send(k_far, CORE_SWAP), send(f_far, CORE_SWAP))
    (att_far,) = attend(ends, qs[:1], state, outs=1)
    back = send(att_far, YH_SWAP)
    q_own, att_far = lax.optimization_barrier((q, att_far))
    att = attend(ends, ((q_own, (0, tok // 2)),), state, offset=2, outs=2)
    peer = [send(att[0], YL_SWAP), send(att[1], YL_SWAP)]
    peer_back = send(back, YL_SWAP)
    pos = jnp.stack([x, yl, yh]).astype(jnp.int32)
    parts = []
    for n in range(2):
        part = mix(pos, (att[n], back, peer[n], peer_back), w_out, w_peer, tokens, out_bias.reshape(1, 128), n)
        here = [part[0]]
        for b, pairs in ((1, X_UP), (2, X_FAR), (3, X_DOWN)):
            here.append(send(part[b], pairs))
        parts.append(here)
    summed = sum(jnp.concatenate([parts[0][b], parts[1][b]], axis=0).astype(f32) for b in range(4))
    return summed.astype(bf16)


def solution(mesh):
    return jax.shard_map(
        per_device,
        mesh=mesh,
        in_specs=(
            P(("rows", "cols"), "heads"),
            P(),
            P(None, None, "heads"),
            P("heads", None),
            P("heads"),
        ),
        out_specs=P(("rows", "cols"), "heads"),
        check_vma=False,
    )
```

```python
import functools

import jax
import jax.numpy as jnp
from jax import lax
from jax.experimental import pallas as pl
from jax.experimental.pallas import tpu as pltpu
from jax.sharding import PartitionSpec as P


D = 1024
HD = 64
LOG2E = 1.4426950408889634
QSCALE = LOG2E / HD**0.5
CAP = 2.0**60
AXES = ("rows", "cols", "heads")
bf16 = jnp.bfloat16
f32 = jnp.float32


def perm(move):
    pairs = []
    for i in range(128):
        here = dict(x=(i % 8) // 2, yl=i % 2, z=(i // 8) % 4, yh=i // 64, c=(i // 32) % 2)
        to = {**here, **move(here)}
        pairs.append((i, ((to["yh"] * 2 + to["c"]) * 4 + to["z"]) * 8 + to["x"] * 2 + to["yl"]))
    return pairs


Z_UP = perm(lambda d: dict(z=(d["z"] + 1) % 4))
Z_DOWN = perm(lambda d: dict(z=(d["z"] - 1) % 4))
Z_BY_CORE = perm(lambda d: dict(z=(d["z"] + 1 - 2 * d["c"]) % 4))
Z_FAR = perm(lambda d: dict(z=(d["z"] + 2) % 4))
YH_SWAP = perm(lambda d: dict(yh=1 - d["yh"]))
YL_SWAP = perm(lambda d: dict(yl=1 - d["yl"]))
CORE_SWAP = perm(lambda d: dict(c=1 - d["c"]))
X_UP = perm(lambda d: dict(x=(d["x"] + 1) % 4))
X_DOWN = perm(lambda d: dict(x=(d["x"] - 1) % 4))
X_FAR = perm(lambda d: dict(x=(d["x"] + 2) % 4))


def send(x, pairs):
    return lax.ppermute(x, AXES, pairs)


def vmem():
    return pl.BlockSpec(memory_space=pltpu.VMEM)


def hbm():
    return pl.BlockSpec(memory_space=pltpu.HBM)


def smem():
    return pl.BlockSpec(memory_space=pltpu.SMEM)


def project_kernel(ids_ref, *refs):
    x_refs = refs[:7]
    halves = refs[7:9]
    gain_ref, w_ref, kv_ref, q_ref, out_ref, n_even, n_odd = refs[9:]
    tok = x_refs[0].shape[0]
    step = 128
    half = tok // 2
    par = ids_ref[8]
    lane = lax.broadcasted_iota(jnp.int32, (step, 128), 1)
    low = lane < HD

    def norm(t, n_ref):
        for part in range(2):
            for r in range(0, step, 32):
                rows = slice(part * half + t * step + r, part * half + t * step + r + 32)
                parts = [x_ref[rows, :].astype(f32) for x_ref in x_refs]
                parts.append(halves[part][t * step + r : t * step + r + 32, :].astype(f32))
                total = parts[0]
                for p in parts[1:]:
                    total = total + p
                mean = jnp.sum(total, axis=1, keepdims=True) * (1.0 / D)
                cs = [p - mean for p in parts]
                sq = cs[0] * cs[0]
                for c in cs[1:]:
                    sq = sq + c * c
                var = jnp.sum(sq, axis=1, keepdims=True) * (1.0 / D)
                inv = lax.rsqrt(var + 1e-06)
                for h in range(8):
                    to = slice(part * step + r, part * step + r + 32)
                    n_ref[ids_ref[h], to] = (cs[h] * inv * gain_ref[ids_ref[h]]).astype(bf16)

    def one(t, n_ref):
        normed = jnp.concatenate([n_ref[h] for h in range(8)], axis=1)
        qk = jnp.dot(normed, jnp.concatenate([w_ref[0], w_ref[1]], axis=1), preferred_element_type=f32)
        v = jnp.dot(normed, w_ref[2], preferred_element_type=f32)
        k0, k1 = qk[:step, 128:], qk[step:, 128:]
        first = jnp.where(low, k0, pltpu.roll(k1, HD, 1))
        second = jnp.where(low, pltpu.roll(k0, HD, 1), k1)
        rows = slice(t * step, (t + 1) * step)
        kv_ref[rows, :] = jnp.where(par > 0, second, first).astype(bf16)
        out_ref[rows, :] = jnp.where(par > 0, first, second).astype(bf16)
        for part in range(2):
            own = slice(part * step, (part + 1) * step)
            block = (part * (half // step) + t) * HD
            vt = v[own].T
            vkeep = jnp.where(par > 0, vt[HD:], vt[:HD])
            vgive = jnp.where(par > 0, vt[:HD], vt[HD:])
            to = slice(half + block, half + block + HD)
            kv_ref[to, :] = vkeep.astype(bf16)
            out_ref[to, :] = vgive.astype(bf16)
            qt = (qk[own, :128] * QSCALE).T
            qkeep = jnp.where(par > 0, qt[HD:], qt[:HD])
            qgive = jnp.where(par > 0, qt[:HD], qt[HD:])
            q_ref[block : block + HD, :] = qkeep.astype(bf16)
            out_ref[tok + block : tok + block + HD, :] = qgive.astype(bf16)

    bufs = (n_even, n_odd)
    trips = half // step
    norm(0, bufs[0])
    for t in range(trips):
        if t + 1 < trips:
            norm(t + 1, bufs[(t + 1) % 2])
        one(t, bufs[t % 2])


def stage_kernel(x_ref, w_ref, xo_ref, wo_ref, sems):
    copies = [
        pltpu.make_async_copy(x_ref, xo_ref, sems.at[0]),
        pltpu.make_async_copy(w_ref, wo_ref, sems.at[1]),
    ]
    for c in copies:
        c.start()
    for c in copies:
        c.wait()


def stage(x, w):
    x, w = (pltpu.with_memory_space_constraint(a, pltpu.HBM) for a in (x, w))
    return pl.pallas_call(
        stage_kernel,
        out_shape=(jax.ShapeDtypeStruct(x.shape, x.dtype), jax.ShapeDtypeStruct(w.shape, w.dtype)),
        in_specs=[hbm(), hbm()],
        out_specs=(vmem(), vmem()),
        scratch_shapes=[pltpu.SemaphoreType.DMA((2,))],
        compiler_params=pltpu.CompilerParams(vmem_limit_bytes=2 << 20),
        name="stage",
    )(x, w)


def project(ids, blocks, gain, w):
    tok = blocks[0].shape[0]
    return pl.pallas_call(
        project_kernel,
        out_shape=(
            jax.ShapeDtypeStruct((tok, 128), bf16),
            jax.ShapeDtypeStruct((tok // 2, 128), bf16),
            jax.ShapeDtypeStruct((tok + tok // 2, 128), bf16),
        ),
        in_specs=[smem()] + [vmem()] * 11,
        out_specs=(vmem(), vmem(), vmem()),
        scratch_shapes=[
            pltpu.VMEM((8, 256, 128), bf16),
            pltpu.VMEM((8, 256, 128), bf16),
        ],
        compiler_params=pltpu.CompilerParams(vmem_limit_bytes=12 << 20),
        name="project",
    )(ids, *blocks, gain, w)


def attend_kernel(*refs, npieces, windows, offset, first, outs, bq, bk, unroll, ahead):
    pieces = refs[:npieces]
    qs = refs[npieces : npieces + len(windows)]
    rest = list(refs[npieces + len(windows) :])
    if not first:
        acc_in, m_in = rest[:2]
        rest = rest[2:]
    out_refs = rest[:outs]
    rest = rest[outs:]
    acc_ref, m_ref, kvs, q2, s = rest
    ntiles = kvs.shape[0]
    per_tile = 1024 // bk
    nkb = ntiles * per_tile
    nqb = q2.shape[0]
    base = 0
    for piece in pieces:
        count = piece.shape[0] // 1024

        def load(i, _, piece=piece, base=base):
            for r in range(0, 1024, 256):
                kvs[base + i, r : r + 256] = piece[pl.ds(pl.multiple_of(i * 1024 + r, 256), 256), :]
            return 0

        lax.fori_loop(0, count, load, 0)
        base += count
    per = bq // 128
    zero = jnp.zeros((HD, bq), bf16)
    jb = 0
    for q, (start, count) in zip(qs, windows):
        for j in range(count // HD // per):
            blocks = [q[start + (j * per + b) * HD : start + (j * per + b + 1) * HD, :] for b in range(per)]
            block = jnp.concatenate(blocks, axis=1)
            q2[jb, 0, 0:HD] = block
            q2[jb, 0, HD:] = zero
            q2[jb, 1, 0:HD] = zero
            q2[jb, 1, HD:] = block
            jb += 1

    def scores(j, i):
        tile, sub = i // per_tile, i % per_tile
        k = kvs[tile, pl.ds(pl.multiple_of(sub * (bk // 2), 128), bk // 2)]
        return [jnp.dot(k, q2[j, e], preferred_element_type=f32) for e in range(2)]

    if first:
        for j in range(nqb):
            top = jnp.dot(kvs[0, 0:128], q2[j, 0], preferred_element_type=f32)
            m_ref[j] = jnp.max(top, axis=0, keepdims=True)
    else:
        for j in range(nqb):
            m_ref[j] = m_in[offset + j]

    def reset(j, _):
        acc_ref[j] = jnp.zeros(acc_ref.shape[1:], f32) if first else acc_in[offset + j]
        return 0

    lax.fori_loop(0, nqb, reset, 0)

    steps = nqb * nkb

    units = [(c, g) for c in range(bk // 256) for g in range(bq // 256)]

    def unit(j, i, c, g):
        tile, sub = i // per_tile, i % per_tile
        half, row = (c * 256) // (bk // 2), (c * 256) % (bk // 2)
        k = kvs[tile, pl.ds(pl.multiple_of(sub * (bk // 2) + row, 128), 256)]
        return jnp.dot(k, q2[j, half, :, g * 256 : (g + 1) * 256], preferred_element_type=f32)

    def values(i, c):
        tile, sub = i // per_tile, i % per_tile
        half, row = (c * 256) // (bk // 2), (c * 256) % (bk // 2)
        at = [512 + (half * 4 + sub * (bk // 256) + row // 128 + b) * HD for b in range(2)]
        return jnp.concatenate([kvs[tile, pl.ds(pl.multiple_of(x, HD), HD)] for x in at], axis=1)

    def trip(t):
        j, i = t // nkb, t % nkb
        u = jnp.where(t + 1 < steps, t + 1, 0)
        todo = [s[n] for n in range(ahead)] if ahead else []
        queue = [(j, i, c, g) for c, g in units]
        later = [(u // nkb, u % nkb, c, g) for c, g in units[:ahead]]
        order = queue[ahead:] + later
        accs = [acc_ref[j, :HD, g * 256 : (g + 1) * 256] for g in range(bq // 256)]
        dens = [acc_ref[j, HD:, g * 256 : (g + 1) * 256] for g in range(bq // 256)]
        tops = [m_ref[j, :, g * 256 : (g + 1) * 256] for g in range(bq // 256)]
        if not ahead:
            todo = [unit(*order.pop(0))]
        made = []
        for n, (jj, ii, c, g) in enumerate(queue):
            if order:
                nxt = unit(*order.pop(0))
                if len(order) < ahead and ahead:
                    made.append(nxt)
                else:
                    todo.append(nxt)
            p = jnp.exp2(todo[n] - tops[g])
            dens[g] = dens[g] + jnp.sum(p.reshape(32, 8, 256), axis=0)
            accs[g] = accs[g] + jnp.dot(values(i, c), p.astype(bf16), preferred_element_type=f32)
        for n, v in enumerate(made):
            s[n] = v
        for g in range(bq // 256):
            acc_ref[j, :HD, g * 256 : (g + 1) * 256] = accs[g]
            acc_ref[j, HD:, g * 256 : (g + 1) * 256] = dens[g]

    def exact(j, _):
        def widen(i, top):
            for part in scores(j, i):
                top = jnp.maximum(top, jnp.max(part, axis=0, keepdims=True))
            return top

        if first:
            top = lax.fori_loop(0, nkb, widen, jnp.full((1, bq), -jnp.inf, f32))
            acc_ref[j] = jnp.zeros(acc_ref.shape[1:], f32)
        else:
            old = m_in[offset + j]
            top = lax.fori_loop(0, nkb, widen, old)
            acc_ref[j] = acc_in[offset + j] * jnp.exp2(old - top)
        m_ref[j] = top
        return 0

    def sweep(turn):
        @pl.when(turn > 0)
        def _():
            lax.fori_loop(0, nqb, exact, 0)

        for n in range(ahead):
            s[n] = unit(0, 0, *units[n])

        def some(h, _):
            for r in range(unroll):
                trip(unroll * h + r)
            return 0

        lax.fori_loop(0, steps // unroll, some, 0)
        den = acc_ref[:, HD:, :]
        fine = jnp.min(jnp.where(den < CAP, 1.0, 0.0)) > 0.5
        return jnp.where(jnp.logical_or(turn > 0, fine), 2, 1)

    lax.while_loop(lambda turn: turn < 2, sweep, 0)

    for n, out_ref in enumerate(out_refs):
        for j in range(nqb // outs):
            a = acc_ref[n * (nqb // outs) + j]
            o = (a[0:HD] * (1.0 / jnp.sum(a[HD:], axis=0, keepdims=True))).astype(bf16)
            for b in range(per):
                out_ref[(j * per + b) * HD : (j * per + b + 1) * HD, :] = o[:, b * 128 : (b + 1) * 128]


def attend(pieces, qs, state=None, offset=0, outs=0, bq=512, bk=1024, unroll=8, ahead=4):
    windows = tuple(w for q, w in qs)
    nkeys = sum(p.shape[0] for p in pieces)
    nqueries = sum(count for start, count in windows) * 2
    nqb = nqueries // bq
    acc_shape = (nqb, HD + 8, bq)
    m_shape = (nqb, 1, bq)
    scratch = [
        pltpu.VMEM((nkeys // 1024, 1024, 128), bf16),
        pltpu.VMEM((nqb, 2, 128, bq), bf16),
        pltpu.VMEM((max(ahead, 1), 256, 256), f32),
    ]
    if outs:
        out_shape = [jax.ShapeDtypeStruct((nqueries // 2 // outs, 128), bf16)] * outs
        out_specs = [vmem()] * outs
        scratch = [pltpu.VMEM(acc_shape, f32), pltpu.VMEM(m_shape, f32)] + scratch
    else:
        out_shape = (jax.ShapeDtypeStruct(acc_shape, f32), jax.ShapeDtypeStruct(m_shape, f32))
        out_specs = (vmem(), vmem())
    args = [*pieces, *(q for q, w in qs)] + ([] if state is None else list(state))
    flops = 4 * nkeys * nqueries * 128
    return pl.pallas_call(
        functools.partial(
            attend_kernel, npieces=len(pieces), windows=windows, offset=offset, first=state is None, outs=outs, bq=bq, bk=bk, unroll=unroll, ahead=ahead
        ),
        out_shape=out_shape,
        in_specs=[vmem()] * len(args),
        out_specs=out_specs,
        scratch_shapes=scratch,
        compiler_params=pltpu.CompilerParams(vmem_limit_bytes=16 << 20),
        cost_estimate=pl.CostEstimate(flops=flops, transcendentals=nkeys * nqueries, bytes_accessed=nkeys * 256),
    )(*args)


def mix_kernel(pos_ref, *refs):
    kept, back, peer_kept, peer_back = refs[:4]
    swap = pos_ref[2] > 0
    own_ref, peer_ref, x_ref, bias_ref = refs[4:8]
    base_ref = refs[8]
    out_refs = refs[9:12]
    w_ref = refs[12]
    for b in range(4):
        cols = pl.ds(pl.multiple_of((((pos_ref[0] + b) % 4) * 2 + pos_ref[1]) * 128, 128), 128)
        w_ref[0:128, b * 128 : (b + 1) * 128] = own_ref[:, cols]
        w_ref[128:256, b * 128 : (b + 1) * 128] = peer_ref[:, cols]

    count = kept.shape[0] // HD

    def one(t, _):
        at = pl.ds(pl.multiple_of(t * HD, HD), HD)
        cols = []
        for mine, other in ((kept, back), (peer_kept, peer_back)):
            a, b = mine[at, :], other[at, :]
            cols += [jnp.where(swap, b, a), jnp.where(swap, a, b)]
        rows = jnp.concatenate(cols, axis=0).T
        out = jnp.dot(rows, w_ref[...], preferred_element_type=f32)
        to = pl.ds(pl.multiple_of(t * 128, 128), 128)
        base_ref[to, :] = out[:, :128] + x_ref[to, :].astype(f32) + bias_ref[...]
        for b in range(3):
            out_refs[b][to, :] = out[:, (b + 1) * 128 : (b + 2) * 128].astype(bf16)
        return 0

    lax.fori_loop(0, count, one, 0, unroll=2)


def mix(pos, att, own, peer, x, bias):
    tok = att[0].shape[0] * 2
    return pl.pallas_call(
        mix_kernel,
        out_shape=[jax.ShapeDtypeStruct((tok, 128), f32)] + [jax.ShapeDtypeStruct((tok, 128), bf16)] * 3,
        in_specs=[smem()] + [vmem()] * 8,
        out_specs=[vmem()] * 4,
        scratch_shapes=[pltpu.VMEM((256, 512), bf16)],
        compiler_params=pltpu.CompilerParams(vmem_limit_bytes=6 << 20),
        name="mix",
    )(pos, *att, own, peer, x, bias)


def per_device(tokens, ln_gain, w_qkv, w_out, out_bias):
    rows = lax.axis_index("rows")
    heads = lax.axis_index("heads")
    yh = rows // 2
    x = heads // 2
    yl = heads % 2
    tok = tokens.shape[0]

    by_y = send(tokens, YL_SWAP)
    by_up = send(tokens, X_UP)
    by_down = send(tokens, X_DOWN)
    y_up = send(by_up, YL_SWAP)
    y_down = send(by_down, YL_SWAP)
    y_far = send(by_y, X_FAR)
    far_lo = send(by_up[: tok // 2], X_UP)
    far_hi = send(by_down[tok // 2 :], X_DOWN)
    held, w_held = stage(tokens, w_qkv)
    blocks = (held, by_up, by_down, by_y, y_up, y_down, y_far, far_lo, far_hi)
    xs = jnp.stack([x, (x + 3) % 4, (x + 1) % 4, (x + 2) % 4])
    ids = jnp.concatenate([xs[:3] * 2 + yl, xs * 2 + 1 - yl, xs[3:] * 2 + yl, yh.reshape(1)]).astype(jnp.int32)

    kv, q, give = project(ids, blocks, ln_gain.reshape(8, 1, 128), w_held)
    got = send(give, YH_SWAP)
    k_other = send(kv, CORE_SWAP)
    k_up = send(kv, Z_UP)
    k_down = send(kv, Z_DOWN)
    kf = got[:tok]
    f_other = send(kf, CORE_SWAP)
    f_up = send(kf, Z_UP)
    f_down = send(kf, Z_DOWN)
    qs = ((got, (tok, tok // 2)), (q, (0, tok // 2)))
    state = attend((kv, kf, k_other, f_other), qs)
    k_up, k_down, f_up, f_down, w_send, state = lax.optimization_barrier((k_up, k_down, f_up, f_down, w_out, state))
    chosen = jnp.where(rows % 2 > 0, jnp.stack([k_down, f_down]), jnp.stack([k_up, f_up]))
    far = send(chosen.reshape(2 * tok, 128), Z_BY_CORE)
    ring = (k_up, k_down, f_up, f_down)
    ring = ring + tuple(send(p, CORE_SWAP) for p in ring)
    w_peer = send(w_send, YL_SWAP)
    state = attend(ring, qs, state)
    ends = (far, send(far, CORE_SWAP))
    (att_far,) = attend(ends, qs[:1], state, outs=1)
    back = send(att_far, YH_SWAP)
    q_own, att_far = lax.optimization_barrier((q, att_far))
    (att,) = attend(ends, ((q_own, (0, tok // 2)),), state, offset=2, outs=1)
    peer = send(att, YL_SWAP)
    peer_back = send(back, YL_SWAP)
    pos = jnp.stack([x, yl, yh]).astype(jnp.int32)
    parts = mix(pos, (att, back, peer, peer_back), w_out, w_peer, tokens, out_bias.reshape(1, 128))
    up = send(parts[1], X_UP)
    across = send(parts[2], X_FAR)
    down = send(parts[3], X_DOWN)
    return (parts[0] + up.astype(f32) + across.astype(f32) + down.astype(f32)).astype(bf16)


def solution(mesh):
    return jax.shard_map(
        per_device,
        mesh=mesh,
        in_specs=(
            P(("rows", "cols"), "heads"),
            P(),
            P(None, None, "heads"),
            P("heads", None),
            P("heads"),
        ),
        out_specs=P(("rows", "cols"), "heads"),
        check_vma=False,
    )
```

```python
import functools

import jax
import jax.numpy as jnp
from jax import lax
from jax.experimental import pallas as pl
from jax.experimental.pallas import tpu as pltpu
from jax.sharding import PartitionSpec as P


D = 1024
HD = 64
LOG2E = 1.4426950408889634
QSCALE = LOG2E / HD**0.5
CAP = 2.0**60
AXES = ("rows", "cols", "heads")
bf16 = jnp.bfloat16
f32 = jnp.float32


def perm(move):
    pairs = []
    for i in range(128):
        here = dict(x=(i % 8) // 2, yl=i % 2, z=(i // 8) % 4, yh=i // 64, c=(i // 32) % 2)
        to = {**here, **move(here)}
        pairs.append((i, ((to["yh"] * 2 + to["c"]) * 4 + to["z"]) * 8 + to["x"] * 2 + to["yl"]))
    return pairs


Z_UP = perm(lambda d: dict(z=(d["z"] + 1) % 4))
Z_DOWN = perm(lambda d: dict(z=(d["z"] - 1) % 4))
Z_BY_CORE = perm(lambda d: dict(z=(d["z"] + 1 - 2 * d["c"]) % 4))
Z_FAR = perm(lambda d: dict(z=(d["z"] + 2) % 4))
YH_SWAP = perm(lambda d: dict(yh=1 - d["yh"]))
YL_SWAP = perm(lambda d: dict(yl=1 - d["yl"]))
CORE_SWAP = perm(lambda d: dict(c=1 - d["c"]))
X_UP = perm(lambda d: dict(x=(d["x"] + 1) % 4))
X_DOWN = perm(lambda d: dict(x=(d["x"] - 1) % 4))
X_FAR = perm(lambda d: dict(x=(d["x"] + 2) % 4))


def send(x, pairs):
    return lax.ppermute(x, AXES, pairs)


def vmem():
    return pl.BlockSpec(memory_space=pltpu.VMEM)


def hbm():
    return pl.BlockSpec(memory_space=pltpu.HBM)


def smem():
    return pl.BlockSpec(memory_space=pltpu.SMEM)


def project_kernel(ids_ref, *refs):
    x_refs = refs[:7]
    halves = refs[7:9]
    gain_ref, w_ref, kv_ref, q_ref, out_ref, qout_ref, n_even, n_odd = refs[9:]
    tok = x_refs[0].shape[0]
    step = 128
    half = tok // 2
    par = ids_ref[8]
    lane = lax.broadcasted_iota(jnp.int32, (step, 128), 1)
    low = lane < HD

    def norm(t, n_ref):
        for part in range(2):
            for r in range(0, step, 32):
                rows = slice(part * half + t * step + r, part * half + t * step + r + 32)
                parts = [x_ref[rows, :].astype(f32) for x_ref in x_refs]
                parts.append(halves[part][t * step + r : t * step + r + 32, :].astype(f32))
                total = parts[0]
                for p in parts[1:]:
                    total = total + p
                mean = jnp.sum(total, axis=1, keepdims=True) * (1.0 / D)
                cs = [p - mean for p in parts]
                sq = cs[0] * cs[0]
                for c in cs[1:]:
                    sq = sq + c * c
                var = jnp.sum(sq, axis=1, keepdims=True) * (1.0 / D)
                inv = lax.rsqrt(var + 1e-06)
                for h in range(8):
                    to = slice(part * step + r, part * step + r + 32)
                    n_ref[ids_ref[h], to] = (cs[h] * inv * gain_ref[ids_ref[h]]).astype(bf16)

    def one(t, n_ref):
        normed = jnp.concatenate([n_ref[h] for h in range(8)], axis=1)
        qk = jnp.dot(normed, jnp.concatenate([w_ref[0], w_ref[1]], axis=1), preferred_element_type=f32)
        v = jnp.dot(normed, w_ref[2], preferred_element_type=f32)
        k0, k1 = qk[:step, 128:], qk[step:, 128:]
        first = jnp.where(low, k0, pltpu.roll(k1, HD, 1))
        second = jnp.where(low, pltpu.roll(k0, HD, 1), k1)
        rows = slice(t * step, (t + 1) * step)
        kv_ref[rows, :] = jnp.where(par > 0, second, first).astype(bf16)
        out_ref[rows, :] = jnp.where(par > 0, first, second).astype(bf16)
        for part in range(2):
            own = slice(part * step, (part + 1) * step)
            block = (part * (half // step) + t) * HD
            vt = v[own].T
            vkeep = jnp.where(par > 0, vt[HD:], vt[:HD])
            vgive = jnp.where(par > 0, vt[:HD], vt[HD:])
            to = slice(half + block, half + block + HD)
            kv_ref[to, :] = vkeep.astype(bf16)
            out_ref[to, :] = vgive.astype(bf16)
            qt = (qk[own, :128] * QSCALE).T
            qkeep = jnp.where(par > 0, qt[HD:], qt[:HD])
            qgive = jnp.where(par > 0, qt[:HD], qt[HD:])
            q_ref[block : block + HD, :] = qkeep.astype(bf16)
            qout_ref[block : block + HD, :] = qgive.astype(bf16)

    bufs = (n_even, n_odd)
    trips = half // step
    norm(0, bufs[0])
    for t in range(trips):
        if t + 1 < trips:
            norm(t + 1, bufs[(t + 1) % 2])
        one(t, bufs[t % 2])


def stage_kernel(x_ref, w_ref, xo_ref, wo_ref, sems):
    copies = [
        pltpu.make_async_copy(x_ref, xo_ref, sems.at[0]),
        pltpu.make_async_copy(w_ref, wo_ref, sems.at[1]),
    ]
    for c in copies:
        c.start()
    for c in copies:
        c.wait()


def stage(x, w):
    x, w = (pltpu.with_memory_space_constraint(a, pltpu.HBM) for a in (x, w))
    return pl.pallas_call(
        stage_kernel,
        out_shape=(jax.ShapeDtypeStruct(x.shape, x.dtype), jax.ShapeDtypeStruct(w.shape, w.dtype)),
        in_specs=[hbm(), hbm()],
        out_specs=(vmem(), vmem()),
        scratch_shapes=[pltpu.SemaphoreType.DMA((2,))],
        compiler_params=pltpu.CompilerParams(vmem_limit_bytes=2 << 20),
        name="stage",
    )(x, w)


def project(ids, blocks, gain, w):
    tok = blocks[0].shape[0]
    return pl.pallas_call(
        project_kernel,
        out_shape=(
            jax.ShapeDtypeStruct((tok, 128), bf16),
            jax.ShapeDtypeStruct((tok // 2, 128), bf16),
            jax.ShapeDtypeStruct((tok, 128), bf16),
            jax.ShapeDtypeStruct((tok // 2, 128), bf16),
        ),
        in_specs=[smem()] + [vmem()] * 11,
        out_specs=(vmem(), vmem(), vmem(), vmem()),
        scratch_shapes=[
            pltpu.VMEM((8, 256, 128), bf16),
            pltpu.VMEM((8, 256, 128), bf16),
        ],
        compiler_params=pltpu.CompilerParams(vmem_limit_bytes=12 << 20),
        name="project",
    )(ids, *blocks, gain, w)


def attend_kernel(*refs, npieces, windows, offset, first, outs, bq, bk, unroll, ahead):
    pieces = refs[:npieces]
    qs = refs[npieces : npieces + len(windows)]
    rest = list(refs[npieces + len(windows) :])
    if not first:
        acc_in, m_in = rest[:2]
        rest = rest[2:]
    out_refs = rest[:outs]
    rest = rest[outs:]
    acc_ref, m_ref, kvs, q2, s = rest
    ntiles = kvs.shape[0]
    per_tile = 1024 // bk
    nkb = ntiles * per_tile
    nqb = q2.shape[0]
    base = 0
    for piece in pieces:
        count = piece.shape[0] // 1024

        def load(i, _, piece=piece, base=base):
            for r in range(0, 1024, 256):
                kvs[base + i, r : r + 256] = piece[pl.ds(pl.multiple_of(i * 1024 + r, 256), 256), :]
            return 0

        lax.fori_loop(0, count, load, 0)
        base += count
    per = bq // 128
    zero = jnp.zeros((HD, bq), bf16)
    jb = 0
    for q, (start, count) in zip(qs, windows):
        for j in range(count // HD // per):
            blocks = [q[start + (j * per + b) * HD : start + (j * per + b + 1) * HD, :] for b in range(per)]
            block = jnp.concatenate(blocks, axis=1)
            q2[jb, 0, 0:HD] = block
            q2[jb, 0, HD:] = zero
            q2[jb, 1, 0:HD] = zero
            q2[jb, 1, HD:] = block
            jb += 1

    def scores(j, i):
        tile, sub = i // per_tile, i % per_tile
        k = kvs[tile, pl.ds(pl.multiple_of(sub * (bk // 2), 128), bk // 2)]
        return [jnp.dot(k, q2[j, e], preferred_element_type=f32) for e in range(2)]

    if first:
        for j in range(nqb):
            top = jnp.dot(kvs[0, 0:128], q2[j, 0], preferred_element_type=f32)
            m_ref[j] = jnp.max(top, axis=0, keepdims=True)
    else:
        for j in range(nqb):
            m_ref[j] = m_in[offset + j]

    def reset(j, _):
        acc_ref[j] = jnp.zeros(acc_ref.shape[1:], f32) if first else acc_in[offset + j]
        return 0

    lax.fori_loop(0, nqb, reset, 0)

    steps = nqb * nkb

    units = [(c, g) for c in range(bk // 256) for g in range(bq // 256)]

    def unit(j, i, c, g):
        tile, sub = i // per_tile, i % per_tile
        half, row = (c * 256) // (bk // 2), (c * 256) % (bk // 2)
        k = kvs[tile, pl.ds(pl.multiple_of(sub * (bk // 2) + row, 128), 256)]
        return jnp.dot(k, q2[j, half, :, g * 256 : (g + 1) * 256], preferred_element_type=f32)

    def values(i, c):
        tile, sub = i // per_tile, i % per_tile
        half, row = (c * 256) // (bk // 2), (c * 256) % (bk // 2)
        at = [512 + (half * 4 + sub * (bk // 256) + row // 128 + b) * HD for b in range(2)]
        return jnp.concatenate([kvs[tile, pl.ds(pl.multiple_of(x, HD), HD)] for x in at], axis=1)

    def trip(t):
        j, i = t // nkb, t % nkb
        u = jnp.where(t + 1 < steps, t + 1, 0)
        todo = [s[n] for n in range(ahead)] if ahead else []
        queue = [(j, i, c, g) for c, g in units]
        later = [(u // nkb, u % nkb, c, g) for c, g in units[:ahead]]
        order = queue[ahead:] + later
        accs = [acc_ref[j, :HD, g * 256 : (g + 1) * 256] for g in range(bq // 256)]
        dens = [acc_ref[j, HD:, g * 256 : (g + 1) * 256] for g in range(bq // 256)]
        tops = [m_ref[j, :, g * 256 : (g + 1) * 256] for g in range(bq // 256)]
        if not ahead:
            todo = [unit(*order.pop(0))]
        made = []
        for n, (jj, ii, c, g) in enumerate(queue):
            if order:
                nxt = unit(*order.pop(0))
                if len(order) < ahead and ahead:
                    made.append(nxt)
                else:
                    todo.append(nxt)
            p = jnp.exp2(todo[n] - tops[g])
            dens[g] = dens[g] + jnp.sum(p.reshape(32, 8, 256), axis=0)
            accs[g] = accs[g] + jnp.dot(values(i, c), p.astype(bf16), preferred_element_type=f32)
        for n, v in enumerate(made):
            s[n] = v
        for g in range(bq // 256):
            acc_ref[j, :HD, g * 256 : (g + 1) * 256] = accs[g]
            acc_ref[j, HD:, g * 256 : (g + 1) * 256] = dens[g]

    def exact(j, _):
        def widen(i, top):
            for part in scores(j, i):
                top = jnp.maximum(top, jnp.max(part, axis=0, keepdims=True))
            return top

        if first:
            top = lax.fori_loop(0, nkb, widen, jnp.full((1, bq), -jnp.inf, f32))
            acc_ref[j] = jnp.zeros(acc_ref.shape[1:], f32)
        else:
            old = m_in[offset + j]
            top = lax.fori_loop(0, nkb, widen, old)
            acc_ref[j] = acc_in[offset + j] * jnp.exp2(old - top)
        m_ref[j] = top
        return 0

    def sweep(turn):
        @pl.when(turn > 0)
        def _():
            lax.fori_loop(0, nqb, exact, 0)

        for n in range(ahead):
            s[n] = unit(0, 0, *units[n])

        def some(h, _):
            for r in range(unroll):
                trip(unroll * h + r)
            return 0

        lax.fori_loop(0, steps // unroll, some, 0)
        den = acc_ref[:, HD:, :]
        fine = jnp.min(jnp.where(den < CAP, 1.0, 0.0)) > 0.5
        return jnp.where(jnp.logical_or(turn > 0, fine), 2, 1)

    lax.while_loop(lambda turn: turn < 2, sweep, 0)

    for n, out_ref in enumerate(out_refs):
        for j in range(nqb // outs):
            a = acc_ref[n * (nqb // outs) + j]
            o = (a[0:HD] * (1.0 / jnp.sum(a[HD:], axis=0, keepdims=True))).astype(bf16)
            for b in range(per):
                out_ref[(j * per + b) * HD : (j * per + b + 1) * HD, :] = o[:, b * 128 : (b + 1) * 128]


def attend(pieces, qs, state=None, offset=0, outs=0, bq=512, bk=1024, unroll=8, ahead=4):
    windows = tuple(w for q, w in qs)
    nkeys = sum(p.shape[0] for p in pieces)
    nqueries = sum(count for start, count in windows) * 2
    nqb = nqueries // bq
    acc_shape = (nqb, HD + 8, bq)
    m_shape = (nqb, 1, bq)
    scratch = [
        pltpu.VMEM((nkeys // 1024, 1024, 128), bf16),
        pltpu.VMEM((nqb, 2, 128, bq), bf16),
        pltpu.VMEM((max(ahead, 1), 256, 256), f32),
    ]
    if outs:
        out_shape = [jax.ShapeDtypeStruct((nqueries // 2 // outs, 128), bf16)] * outs
        out_specs = [vmem()] * outs
        scratch = [pltpu.VMEM(acc_shape, f32), pltpu.VMEM(m_shape, f32)] + scratch
    else:
        out_shape = (jax.ShapeDtypeStruct(acc_shape, f32), jax.ShapeDtypeStruct(m_shape, f32))
        out_specs = (vmem(), vmem())
    args = [*pieces, *(q for q, w in qs)] + ([] if state is None else list(state))
    flops = 4 * nkeys * nqueries * 128
    return pl.pallas_call(
        functools.partial(
            attend_kernel, npieces=len(pieces), windows=windows, offset=offset, first=state is None, outs=outs, bq=bq, bk=bk, unroll=unroll, ahead=ahead
        ),
        out_shape=out_shape,
        in_specs=[vmem()] * len(args),
        out_specs=out_specs,
        scratch_shapes=scratch,
        compiler_params=pltpu.CompilerParams(vmem_limit_bytes=16 << 20),
        cost_estimate=pl.CostEstimate(flops=flops, transcendentals=nkeys * nqueries, bytes_accessed=nkeys * 256),
    )(*args)


def columns_of(att_refs, t, swap):
    kept, back, peer_kept, peer_back = att_refs
    at = pl.ds(pl.multiple_of(t * HD, HD), HD)
    cols = []
    for mine, other in ((kept, back), (peer_kept, peer_back)):
        a, b = mine[at, :], other[at, :]
        cols += [jnp.where(swap, b, a), jnp.where(swap, a, b)]
    return jnp.concatenate(cols, axis=0).T


def weights_for(pos_ref, own_ref, peer_ref, w_ref, steps):
    for n, b in enumerate(steps):
        cols = pl.ds(pl.multiple_of((((pos_ref[0] + b) % 4) * 2 + pos_ref[1]) * 128, 128), 128)
        w_ref[0:128, n * 128 : (n + 1) * 128] = own_ref[:, cols]
        w_ref[128:256, n * 128 : (n + 1) * 128] = peer_ref[:, cols]


def far_kernel(pos_ref, *refs):
    att_refs, (own_ref, peer_ref, lo_ref, hi_ref, t_ref, w_ref) = refs[:4], refs[4:]
    weights_for(pos_ref, own_ref, peer_ref, w_ref, (2,))
    swap = pos_ref[2] > 0
    count = att_refs[0].shape[0] // HD
    for t in range(count):
        rows = columns_of(att_refs, t, swap)
        t_ref[t] = rows
        out = jnp.dot(rows, w_ref[...], preferred_element_type=f32).astype(bf16)
        half = (lo_ref, hi_ref)[t // (count // 2)]
        to = (t % (count // 2)) * 128
        half[to : to + 128, :] = out


def mix_far(pos, att, own, peer):
    tok = att[0].shape[0] * 2
    return pl.pallas_call(
        far_kernel,
        out_shape=[jax.ShapeDtypeStruct((tok // 2, 128), bf16)] * 2
        + [jax.ShapeDtypeStruct((tok // 128, 128, 256), bf16)],
        in_specs=[smem()] + [vmem()] * 6,
        out_specs=[vmem()] * 3,
        scratch_shapes=[pltpu.VMEM((256, 128), bf16)],
        compiler_params=pltpu.CompilerParams(vmem_limit_bytes=6 << 20),
        name="mix_far",
    )(pos, *att, own, peer)


def mix_kernel(pos_ref, rows_ref, own_ref, peer_ref, x_ref, bias_ref, base_ref, up_ref, down_ref, w_ref):
    weights_for(pos_ref, own_ref, peer_ref, w_ref, (0, 1, 3))

    def one(t, _):
        out = jnp.dot(rows_ref[t], w_ref[...], preferred_element_type=f32)
        to = pl.ds(pl.multiple_of(t * 128, 128), 128)
        base_ref[to, :] = out[:, :128] + x_ref[to, :].astype(f32) + bias_ref[...]
        up_ref[to, :] = out[:, 128:256].astype(bf16)
        down_ref[to, :] = out[:, 256:].astype(bf16)
        return 0

    lax.fori_loop(0, rows_ref.shape[0], one, 0, unroll=4)


def mix(pos, rows, own, peer, x, bias):
    return pl.pallas_call(
        mix_kernel,
        out_shape=[jax.ShapeDtypeStruct(x.shape, f32)] + [jax.ShapeDtypeStruct(x.shape, bf16)] * 2,
        in_specs=[smem()] + [vmem()] * 5,
        out_specs=[vmem()] * 3,
        scratch_shapes=[pltpu.VMEM((256, 384), bf16)],
        compiler_params=pltpu.CompilerParams(vmem_limit_bytes=6 << 20),
        name="mix",
    )(pos, rows, own, peer, x, bias)


def join_kernel(up_ref, down_ref, lo_ref, hi_ref, upo_ref, downo_ref):
    half = lo_ref.shape[0]
    upo_ref[:half] = (up_ref[:half].astype(f32) + lo_ref[...].astype(f32)).astype(bf16)
    upo_ref[half:] = up_ref[half:]
    downo_ref[:half] = down_ref[:half]
    downo_ref[half:] = (down_ref[half:].astype(f32) + hi_ref[...].astype(f32)).astype(bf16)


def join(up, down, lo, hi):
    return pl.pallas_call(
        join_kernel,
        out_shape=[jax.ShapeDtypeStruct(up.shape, bf16)] * 2,
        in_specs=[vmem()] * 4,
        out_specs=[vmem()] * 2,
        compiler_params=pltpu.CompilerParams(vmem_limit_bytes=6 << 20),
        name="join",
    )(up, down, lo, hi)


def per_device(tokens, ln_gain, w_qkv, w_out, out_bias):
    rows = lax.axis_index("rows")
    heads = lax.axis_index("heads")
    yh = rows // 2
    x = heads // 2
    yl = heads % 2
    tok = tokens.shape[0]

    by_y = send(tokens, YL_SWAP)
    by_up = send(tokens, X_UP)
    by_down = send(tokens, X_DOWN)
    y_up = send(by_up, YL_SWAP)
    y_down = send(by_down, YL_SWAP)
    y_far = send(by_y, X_FAR)
    far_lo = send(by_up[: tok // 2], X_UP)
    far_hi = send(by_down[tok // 2 :], X_DOWN)
    held, w_held = stage(tokens, w_qkv)
    blocks = (held, by_up, by_down, by_y, y_up, y_down, y_far, far_lo, far_hi)
    xs = jnp.stack([x, (x + 3) % 4, (x + 1) % 4, (x + 2) % 4])
    ids = jnp.concatenate([xs[:3] * 2 + yl, xs * 2 + 1 - yl, xs[3:] * 2 + yl, yh.reshape(1)]).astype(jnp.int32)

    kv, q, give, give_q = project(ids, blocks, ln_gain.reshape(8, 1, 128), w_held)
    kf = send(give, YH_SWAP)
    q_far = send(give_q, YH_SWAP)
    k_other = send(kv, CORE_SWAP)
    k_up = send(kv, Z_UP)
    k_down = send(kv, Z_DOWN)
    f_other = send(kf, CORE_SWAP)
    f_up = send(kf, Z_UP)
    f_down = send(kf, Z_DOWN)
    qs = ((q_far, (0, tok // 2)), (q, (0, tok // 2)))
    state = attend((kv, kf, k_other, f_other), qs)
    k_up, k_down, f_up, f_down, w_send, state = lax.optimization_barrier((k_up, k_down, f_up, f_down, w_out, state))
    chosen = jnp.where(rows % 2 > 0, jnp.stack([k_down, f_down]), jnp.stack([k_up, f_up]))
    far = send(chosen.reshape(2 * tok, 128), Z_BY_CORE)
    ring = (k_up, k_down, f_up, f_down)
    ring = ring + tuple(send(p, CORE_SWAP) for p in ring)
    w_peer = send(w_send, YL_SWAP)
    state = attend(ring, qs, state)
    ends = (far, send(far, CORE_SWAP))
    (att_far,) = attend(ends, qs[:1], state, outs=1)
    back = send(att_far, YH_SWAP)
    q_own, att_far = lax.optimization_barrier((q, att_far))
    (att,) = attend(ends, ((q_own, (0, tok // 2)),), state, offset=2, outs=1)
    peer = send(att, YL_SWAP)
    peer_back = send(back, YL_SWAP)
    pos = jnp.stack([x, yl, yh]).astype(jnp.int32)
    lo, hi, att_rows = mix_far(pos, (att, back, peer, peer_back), w_out, w_peer)
    lo = send(lo, X_UP)
    hi = send(hi, X_DOWN)
    base, up, down = mix(pos, att_rows, w_out, w_peer, tokens, out_bias.reshape(1, 128))
    up, down = join(up, down, lo, hi)
    up = send(up, X_UP)
    down = send(down, X_DOWN)
    return (base + up.astype(f32) + down.astype(f32)).astype(bf16)


def solution(mesh):
    return jax.shard_map(
        per_device,
        mesh=mesh,
        in_specs=(
            P(("rows", "cols"), "heads"),
            P(),
            P(None, None, "heads"),
            P("heads", None),
            P("heads"),
        ),
        out_specs=P(("rows", "cols"), "heads"),
        check_vma=False,
    )
```

```python
import functools

import jax
import jax.numpy as jnp
from jax import lax
from jax.experimental import pallas as pl
from jax.experimental.pallas import tpu as pltpu
from jax.sharding import PartitionSpec as P


D = 1024
HD = 64
LOG2E = 1.4426950408889634
QSCALE = LOG2E / HD**0.5
CAP = 2.0**60
AXES = ("rows", "cols", "heads")
bf16 = jnp.bfloat16
f32 = jnp.float32


def perm(move):
    pairs = []
    for i in range(128):
        here = dict(x=(i % 8) // 2, yl=i % 2, z=(i // 8) % 4, yh=i // 64, c=(i // 32) % 2)
        to = {**here, **move(here)}
        pairs.append((i, ((to["yh"] * 2 + to["c"]) * 4 + to["z"]) * 8 + to["x"] * 2 + to["yl"]))
    return pairs


Z_UP = perm(lambda d: dict(z=(d["z"] + 1) % 4))
Z_DOWN = perm(lambda d: dict(z=(d["z"] - 1) % 4))
Z_BY_CORE = perm(lambda d: dict(z=(d["z"] + 1 - 2 * d["c"]) % 4))
Z_FAR = perm(lambda d: dict(z=(d["z"] + 2) % 4))
YH_SWAP = perm(lambda d: dict(yh=1 - d["yh"]))
YL_SWAP = perm(lambda d: dict(yl=1 - d["yl"]))
CORE_SWAP = perm(lambda d: dict(c=1 - d["c"]))
X_UP = perm(lambda d: dict(x=(d["x"] + 1) % 4))
X_DOWN = perm(lambda d: dict(x=(d["x"] - 1) % 4))
X_FAR = perm(lambda d: dict(x=(d["x"] + 2) % 4))


def send(x, pairs):
    return lax.ppermute(x, AXES, pairs)


def vmem():
    return pl.BlockSpec(memory_space=pltpu.VMEM)


def hbm():
    return pl.BlockSpec(memory_space=pltpu.HBM)


def smem():
    return pl.BlockSpec(memory_space=pltpu.SMEM)


def project_kernel(ids_ref, *refs):
    x_refs = refs[:7]
    halves = refs[7:9]
    gain_ref, w_ref, kv_ref, q_ref, out_ref, qout_ref, n_even, n_odd = refs[9:]
    tok = x_refs[0].shape[0]
    step = 128
    half = tok // 2
    par = ids_ref[8]
    lane = lax.broadcasted_iota(jnp.int32, (step, 128), 1)
    low = lane < HD

    def norm(t, n_ref):
        for part in range(2):
            for r in range(0, step, 32):
                rows = slice(part * half + t * step + r, part * half + t * step + r + 32)
                parts = [x_ref[rows, :].astype(f32) for x_ref in x_refs]
                parts.append(halves[part][t * step + r : t * step + r + 32, :].astype(f32))
                total = parts[0]
                for p in parts[1:]:
                    total = total + p
                mean = jnp.sum(total, axis=1, keepdims=True) * (1.0 / D)
                cs = [p - mean for p in parts]
                sq = cs[0] * cs[0]
                for c in cs[1:]:
                    sq = sq + c * c
                var = jnp.sum(sq, axis=1, keepdims=True) * (1.0 / D)
                inv = lax.rsqrt(var + 1e-06)
                for h in range(8):
                    to = slice(part * step + r, part * step + r + 32)
                    n_ref[ids_ref[h], to] = (cs[h] * inv * gain_ref[ids_ref[h]]).astype(bf16)

    def one(t, n_ref):
        normed = jnp.concatenate([n_ref[h] for h in range(8)], axis=1)
        qk = jnp.dot(normed, jnp.concatenate([w_ref[0], w_ref[1]], axis=1), preferred_element_type=f32)
        v = jnp.dot(normed, w_ref[2], preferred_element_type=f32)
        k0, k1 = qk[:step, 128:], qk[step:, 128:]
        first = jnp.where(low, k0, pltpu.roll(k1, HD, 1))
        second = jnp.where(low, pltpu.roll(k0, HD, 1), k1)
        rows = slice(t * step, (t + 1) * step)
        kv_ref[rows, :] = jnp.where(par > 0, second, first).astype(bf16)
        out_ref[rows, :] = jnp.where(par > 0, first, second).astype(bf16)
        for part in range(2):
            own = slice(part * step, (part + 1) * step)
            block = (part * (half // step) + t) * HD
            vt = v[own].T
            vkeep = jnp.where(par > 0, vt[HD:], vt[:HD])
            vgive = jnp.where(par > 0, vt[:HD], vt[HD:])
            to = slice(half + block, half + block + HD)
            kv_ref[to, :] = vkeep.astype(bf16)
            out_ref[to, :] = vgive.astype(bf16)
            qt = (qk[own, :128] * QSCALE).T
            qkeep = jnp.where(par > 0, qt[HD:], qt[:HD])
            qgive = jnp.where(par > 0, qt[:HD], qt[HD:])
            q_ref[block : block + HD, :] = qkeep.astype(bf16)
            qout_ref[block : block + HD, :] = qgive.astype(bf16)

    bufs = (n_even, n_odd)
    trips = half // step
    norm(0, bufs[0])
    for t in range(trips):
        if t + 1 < trips:
            norm(t + 1, bufs[(t + 1) % 2])
        one(t, bufs[t % 2])


def stage_kernel(*refs):
    sems = refs[-1]
    count = len(refs) // 2
    copies = [pltpu.make_async_copy(refs[n], refs[count + n], sems.at[n]) for n in range(count)]
    for c in copies:
        c.start()
    for c in copies:
        c.wait()


def stage(*arrays):
    arrays = [pltpu.with_memory_space_constraint(a, pltpu.HBM) for a in arrays]
    return pl.pallas_call(
        stage_kernel,
        out_shape=[jax.ShapeDtypeStruct(a.shape, a.dtype) for a in arrays],
        in_specs=[hbm() for a in arrays],
        out_specs=[vmem() for a in arrays],
        scratch_shapes=[pltpu.SemaphoreType.DMA((len(arrays),))],
        compiler_params=pltpu.CompilerParams(vmem_limit_bytes=2 << 20),
        name="stage",
    )(*arrays)


def project(ids, blocks, gain, w):
    tok = blocks[0].shape[0]
    return pl.pallas_call(
        project_kernel,
        out_shape=(
            jax.ShapeDtypeStruct((tok, 128), bf16),
            jax.ShapeDtypeStruct((tok // 2, 128), bf16),
            jax.ShapeDtypeStruct((tok, 128), bf16),
            jax.ShapeDtypeStruct((tok // 2, 128), bf16),
        ),
        in_specs=[smem()] + [vmem()] * 11,
        out_specs=(vmem(), vmem(), vmem(), vmem()),
        scratch_shapes=[
            pltpu.VMEM((8, 256, 128), bf16),
            pltpu.VMEM((8, 256, 128), bf16),
        ],
        compiler_params=pltpu.CompilerParams(vmem_limit_bytes=12 << 20),
        name="project",
    )(ids, *blocks, gain, w)


def attend_kernel(*refs, npieces, windows, offset, first, outs, bq, unroll, ahead):
    pieces = refs[:npieces]
    qs = refs[npieces : npieces + len(windows)]
    rest = list(refs[npieces + len(windows) :])
    if not first:
        acc_in, m_in = rest[:2]
        rest = rest[2:]
    out_refs = rest[:outs]
    rest = rest[outs:]
    acc_ref, m_ref, q2, s = rest
    tiles = [(p, r) for p in pieces for r in range(0, p.shape[0], 1024)]
    nkb = len(tiles)
    nqb = q2.shape[0]
    per = bq // 128
    zero = jnp.zeros((HD, bq), bf16)
    jb = 0
    for q, (start, count) in zip(qs, windows):
        for j in range(count // HD // per):
            blocks = [q[start + (j * per + b) * HD : start + (j * per + b + 1) * HD, :] for b in range(per)]
            block = jnp.concatenate(blocks, axis=1)
            q2[jb, 0, 0:HD] = block
            q2[jb, 0, HD:] = zero
            q2[jb, 1, 0:HD] = zero
            q2[jb, 1, HD:] = block
            jb += 1

    if first:
        for j in range(nqb):
            top = jnp.dot(tiles[0][0][0:128], q2[j, 0], preferred_element_type=f32)
            m_ref[j] = jnp.max(top, axis=0, keepdims=True)
    else:
        for j in range(nqb):
            m_ref[j] = m_in[offset + j]

    def reset(j, _):
        acc_ref[j] = jnp.zeros(acc_ref.shape[1:], f32) if first else acc_in[offset + j]
        return 0

    lax.fori_loop(0, nqb, reset, 0)

    blocks = unroll // nkb
    units = [(d, i, c, g) for d in range(blocks) for i in range(nkb) for c in range(4) for g in range(bq // 256)]

    def unit(j, i, c, g):
        piece, row = tiles[i]
        half, at = c // 2, row + (c % 2) * 256
        k = piece[at : at + 256, :]
        return jnp.dot(k, q2[j, half, :, g * 256 : (g + 1) * 256], preferred_element_type=f32)

    def values(i, c):
        piece, row = tiles[i]
        at = [row + 512 + (c * 2 + b) * HD for b in range(2)]
        return jnp.concatenate([piece[r : r + HD, :] for r in at], axis=1)

    def trip(h):
        base = h * blocks
        then = jnp.where(base + blocks < nqb, base + blocks, 0)
        todo = [s[n] for n in range(ahead)]
        order = [(base + d, i, c, g) for d, i, c, g in units[ahead:]]
        order += [(then + d, i, c, g) for d, i, c, g in units[:ahead]]
        state = {}
        for n, (d, i, c, g) in enumerate(units):
            made = unit(*order[n])
            if n < len(units) - ahead:
                todo.append(made)
            else:
                s[n - (len(units) - ahead)] = made
            at = slice(g * 256, (g + 1) * 256)
            if (d, g) not in state:
                state[d, g] = [acc_ref[base + d, :HD, at], acc_ref[base + d, HD:, at], m_ref[base + d, :, at]]
            acc, den, top = state[d, g]
            p = jnp.exp2(todo[n] - top)
            den = den + jnp.sum(p.reshape(32, 8, 256), axis=0)
            acc = acc + jnp.dot(values(i, c), p.astype(bf16), preferred_element_type=f32)
            state[d, g] = [acc, den, top]
            if i == nkb - 1 and c == 3:
                acc_ref[base + d, :HD, at] = acc
                acc_ref[base + d, HD:, at] = den

    def exact(j, _):
        top = jnp.full((1, bq), -jnp.inf, f32) if first else m_in[offset + j]
        for piece, row in tiles:
            for half in range(2):

                def widen(r, top, piece=piece, row=row, half=half):
                    k = piece[pl.ds(pl.multiple_of(row + r * 128, 128), 128), :]
                    part = jnp.dot(k, q2[j, half], preferred_element_type=f32)
                    return jnp.maximum(top, jnp.max(part, axis=0, keepdims=True))

                top = lax.fori_loop(0, 4, widen, top)
        if first:
            acc_ref[j] = jnp.zeros(acc_ref.shape[1:], f32)
        else:
            acc_ref[j] = acc_in[offset + j] * jnp.exp2(m_in[offset + j] - top)
        m_ref[j] = top
        return 0

    def sweep(turn):
        @pl.when(turn > 0)
        def _():
            lax.fori_loop(0, nqb, exact, 0)

        for n in range(ahead):
            s[n] = unit(*units[n])

        def some(h, _):
            trip(h)
            return 0

        lax.fori_loop(0, nqb // blocks, some, 0)
        den = acc_ref[:, HD:, :]
        fine = jnp.min(jnp.where(den < CAP, 1.0, 0.0)) > 0.5
        return jnp.where(jnp.logical_or(turn > 0, fine), 2, 1)

    lax.while_loop(lambda turn: turn < 2, sweep, 0)

    for n, out_ref in enumerate(out_refs):
        for j in range(nqb // outs):
            a = acc_ref[n * (nqb // outs) + j]
            o = (a[0:HD] * (1.0 / jnp.sum(a[HD:], axis=0, keepdims=True))).astype(bf16)
            for b in range(per):
                out_ref[(j * per + b) * HD : (j * per + b + 1) * HD, :] = o[:, b * 128 : (b + 1) * 128]


def attend(pieces, qs, state=None, offset=0, outs=0, bq=512, unroll=8, ahead=4):
    windows = tuple(w for q, w in qs)
    nkeys = sum(p.shape[0] for p in pieces)
    nqueries = sum(count for start, count in windows) * 2
    nqb = nqueries // bq
    acc_shape = (nqb, HD + 8, bq)
    m_shape = (nqb, 1, bq)
    scratch = [
        pltpu.VMEM((nqb, 2, 128, bq), bf16),
        pltpu.VMEM((max(ahead, 1), 256, 256), f32),
    ]
    if outs:
        out_shape = [jax.ShapeDtypeStruct((nqueries // 2 // outs, 128), bf16)] * outs
        out_specs = [vmem()] * outs
        scratch = [pltpu.VMEM(acc_shape, f32), pltpu.VMEM(m_shape, f32)] + scratch
    else:
        out_shape = (jax.ShapeDtypeStruct(acc_shape, f32), jax.ShapeDtypeStruct(m_shape, f32))
        out_specs = (vmem(), vmem())
    args = [*pieces, *(q for q, w in qs)] + ([] if state is None else list(state))
    flops = 4 * nkeys * nqueries * 128
    return pl.pallas_call(
        functools.partial(
            attend_kernel, npieces=len(pieces), windows=windows, offset=offset, first=state is None, outs=outs, bq=bq, unroll=unroll, ahead=ahead
        ),
        out_shape=out_shape,
        in_specs=[vmem()] * len(args),
        out_specs=out_specs,
        scratch_shapes=scratch,
        compiler_params=pltpu.CompilerParams(vmem_limit_bytes=16 << 20),
        cost_estimate=pl.CostEstimate(flops=flops, transcendentals=nkeys * nqueries, bytes_accessed=nkeys * 256),
    )(*args)


def columns_of(att_refs, t, swap):
    kept, back, peer_kept, peer_back = att_refs
    at = pl.ds(pl.multiple_of(t * HD, HD), HD)
    cols = []
    for mine, other in ((kept, back), (peer_kept, peer_back)):
        a, b = mine[at, :], other[at, :]
        cols += [jnp.where(swap, b, a), jnp.where(swap, a, b)]
    return jnp.concatenate(cols, axis=0).T


def weights_for(pos_ref, own_ref, peer_ref, w_ref, steps):
    for n, b in enumerate(steps):
        cols = pl.ds(pl.multiple_of((((pos_ref[0] + b) % 4) * 2 + pos_ref[1]) * 128, 128), 128)
        w_ref[0:128, n * 128 : (n + 1) * 128] = own_ref[:, cols]
        w_ref[128:256, n * 128 : (n + 1) * 128] = peer_ref[:, cols]


def far_kernel(pos_ref, *refs):
    att_refs, (own_ref, peer_ref, lo_ref, hi_ref, t_ref, w_ref) = refs[:4], refs[4:]
    weights_for(pos_ref, own_ref, peer_ref, w_ref, (2,))
    swap = pos_ref[2] > 0
    count = att_refs[0].shape[0] // HD
    for t in range(count):
        rows = columns_of(att_refs, t, swap)
        t_ref[t] = rows
        out = jnp.dot(rows, w_ref[...], preferred_element_type=f32).astype(bf16)
        half = (lo_ref, hi_ref)[t // (count // 2)]
        to = (t % (count // 2)) * 128
        half[to : to + 128, :] = out


def mix_far(pos, att, own, peer):
    tok = att[0].shape[0] * 2
    return pl.pallas_call(
        far_kernel,
        out_shape=[jax.ShapeDtypeStruct((tok // 2, 128), bf16)] * 2
        + [jax.ShapeDtypeStruct((tok // 128, 128, 256), bf16)],
        in_specs=[smem()] + [vmem()] * 6,
        out_specs=[vmem()] * 3,
        scratch_shapes=[pltpu.VMEM((256, 128), bf16)],
        compiler_params=pltpu.CompilerParams(vmem_limit_bytes=6 << 20),
        name="mix_far",
    )(pos, *att, own, peer)


def mix_kernel(pos_ref, rows_ref, own_ref, peer_ref, x_ref, bias_ref, base_ref, up_ref, down_ref, w_ref):
    weights_for(pos_ref, own_ref, peer_ref, w_ref, (0, 1, 3))

    def one(t, _):
        out = jnp.dot(rows_ref[t], w_ref[...], preferred_element_type=f32)
        to = pl.ds(pl.multiple_of(t * 128, 128), 128)
        base_ref[to, :] = out[:, :128] + x_ref[to, :].astype(f32) + bias_ref[...]
        up_ref[to, :] = out[:, 128:256].astype(bf16)
        down_ref[to, :] = out[:, 256:].astype(bf16)
        return 0

    lax.fori_loop(0, rows_ref.shape[0], one, 0, unroll=4)


def mix(pos, rows, own, peer, x, bias):
    return pl.pallas_call(
        mix_kernel,
        out_shape=[jax.ShapeDtypeStruct(x.shape, f32)] + [jax.ShapeDtypeStruct(x.shape, bf16)] * 2,
        in_specs=[smem()] + [vmem()] * 5,
        out_specs=[vmem()] * 3,
        scratch_shapes=[pltpu.VMEM((256, 384), bf16)],
        compiler_params=pltpu.CompilerParams(vmem_limit_bytes=6 << 20),
        name="mix",
    )(pos, rows, own, peer, x, bias)


def join_kernel(up_ref, down_ref, lo_ref, hi_ref, upo_ref, downo_ref):
    half = lo_ref.shape[0]
    upo_ref[:half] = (up_ref[:half].astype(f32) + lo_ref[...].astype(f32)).astype(bf16)
    upo_ref[half:] = up_ref[half:]
    downo_ref[:half] = down_ref[:half]
    downo_ref[half:] = (down_ref[half:].astype(f32) + hi_ref[...].astype(f32)).astype(bf16)


def join(up, down, lo, hi):
    return pl.pallas_call(
        join_kernel,
        out_shape=[jax.ShapeDtypeStruct(up.shape, bf16)] * 2,
        in_specs=[vmem()] * 4,
        out_specs=[vmem()] * 2,
        compiler_params=pltpu.CompilerParams(vmem_limit_bytes=6 << 20),
        name="join",
    )(up, down, lo, hi)


def per_device(tokens, ln_gain, w_qkv, w_out, out_bias):
    rows = lax.axis_index("rows")
    heads = lax.axis_index("heads")
    yh = rows // 2
    x = heads // 2
    yl = heads % 2
    tok = tokens.shape[0]

    by_y = send(tokens, YL_SWAP)
    by_up = send(tokens, X_UP)
    by_down = send(tokens, X_DOWN)
    y_up = send(by_up, YL_SWAP)
    y_down = send(by_down, YL_SWAP)
    y_far = send(by_y, X_FAR)
    far_lo = send(by_up[: tok // 2], X_UP)
    far_hi = send(by_down[tok // 2 :], X_DOWN)
    held, w_held, bias = stage(tokens, w_qkv, out_bias.reshape(1, 128))
    blocks = (held, by_up, by_down, by_y, y_up, y_down, y_far, far_lo, far_hi)
    xs = jnp.stack([x, (x + 3) % 4, (x + 1) % 4, (x + 2) % 4])
    ids = jnp.concatenate([xs[:3] * 2 + yl, xs * 2 + 1 - yl, xs[3:] * 2 + yl, yh.reshape(1)]).astype(jnp.int32)

    kv, q, give, give_q = project(ids, blocks, ln_gain.reshape(8, 1, 128), w_held)
    kf = send(give, YH_SWAP)
    q_far = send(give_q, YH_SWAP)
    k_other = send(kv, CORE_SWAP)
    k_up = send(kv, Z_UP)
    k_down = send(kv, Z_DOWN)
    f_other = send(kf, CORE_SWAP)
    f_ring = send(jnp.concatenate([kf, f_other], axis=0), Z_BY_CORE)
    qs = ((q_far, (0, tok // 2)), (q, (0, tok // 2)))
    state = attend((kv, kf, k_other, f_other), qs)
    k_up, k_down, f_ring, w_send, state = lax.optimization_barrier((k_up, k_down, f_ring, w_out, state))
    far = jnp.concatenate([jnp.where(rows % 2 > 0, k_down, k_up), f_ring[:tok]], axis=0)
    far = send(far, Z_BY_CORE)
    ring = (k_up, k_down, f_ring)
    ring = ring + tuple(send(p, CORE_SWAP) for p in ring)
    w_peer = send(w_send, YL_SWAP)
    state_far = attend(ring, qs[:1], state)
    ends = (far, send(far, CORE_SWAP))
    (att_far,) = attend(ends, qs[:1], state_far, outs=1)
    back = send(att_far, YH_SWAP)
    q_own, att_far = lax.optimization_barrier((q, att_far))
    qs_own = ((q_own, (0, tok // 2)),)
    state_own = attend(ring, qs_own, state, offset=2)
    peer_back = send(back, YL_SWAP)
    (att,) = attend(ends, qs_own, state_own, outs=1)
    peer = send(att, YL_SWAP)
    pos = jnp.stack([x, yl, yh]).astype(jnp.int32)
    lo, hi, att_rows = mix_far(pos, (att, back, peer, peer_back), w_out, w_peer)
    lo = send(lo, X_UP)
    hi = send(hi, X_DOWN)
    base, up, down = mix(pos, att_rows, w_out, w_peer, tokens, bias)
    up, down = join(up, down, lo, hi)
    up = send(up, X_UP)
    down = send(down, X_DOWN)
    return (base + up.astype(f32) + down.astype(f32)).astype(bf16)


def solution(mesh):
    return jax.shard_map(
        per_device,
        mesh=mesh,
        in_specs=(
            P(("rows", "cols"), "heads"),
            P(),
            P(None, None, "heads"),
            P("heads", None),
            P("heads"),
        ),
        out_specs=P(("rows", "cols"), "heads"),
        check_vma=False,
    )
```

```python
import functools

import jax
import jax.numpy as jnp
from jax import lax
from jax.experimental import pallas as pl
from jax.experimental.pallas import tpu as pltpu
from jax.sharding import PartitionSpec as P


D = 1024
HD = 64
LOG2E = 1.4426950408889634
QSCALE = LOG2E / HD**0.5
CAP = 2.0**60
AXES = ("rows", "cols", "heads")
bf16 = jnp.bfloat16
f32 = jnp.float32


def perm(move):
    pairs = []
    for i in range(128):
        here = dict(x=(i % 8) // 2, yl=i % 2, z=(i // 8) % 4, yh=i // 64, c=(i // 32) % 2)
        to = {**here, **move(here)}
        pairs.append((i, ((to["yh"] * 2 + to["c"]) * 4 + to["z"]) * 8 + to["x"] * 2 + to["yl"]))
    return pairs


Z_UP = perm(lambda d: dict(z=(d["z"] + 1) % 4))
Z_DOWN = perm(lambda d: dict(z=(d["z"] - 1) % 4))
Z_BY_CORE = perm(lambda d: dict(z=(d["z"] + 1 - 2 * d["c"]) % 4))
Z_FAR = perm(lambda d: dict(z=(d["z"] + 2) % 4))
YH_SWAP = perm(lambda d: dict(yh=1 - d["yh"]))
YL_SWAP = perm(lambda d: dict(yl=1 - d["yl"]))
CORE_SWAP = perm(lambda d: dict(c=1 - d["c"]))
X_UP = perm(lambda d: dict(x=(d["x"] + 1) % 4))
X_DOWN = perm(lambda d: dict(x=(d["x"] - 1) % 4))
X_FAR = perm(lambda d: dict(x=(d["x"] + 2) % 4))


def send(x, pairs):
    return lax.ppermute(x, AXES, pairs)


def vmem():
    return pl.BlockSpec(memory_space=pltpu.VMEM)


def hbm():
    return pl.BlockSpec(memory_space=pltpu.HBM)


def smem():
    return pl.BlockSpec(memory_space=pltpu.SMEM)


def project_kernel(ids_ref, *refs):
    x_refs = refs[:7]
    halves = refs[7:9]
    gain_ref, w_ref, kv_ref, q_ref, out_ref, qout_ref, n_even, n_odd = refs[9:]
    tok = x_refs[0].shape[0]
    step = 128
    half = tok // 2
    par = ids_ref[8]
    lane = lax.broadcasted_iota(jnp.int32, (step, 128), 1)
    low = lane < HD

    def norm(t, n_ref):
        for part in range(2):
            for r in range(0, step, 32):
                rows = slice(part * half + t * step + r, part * half + t * step + r + 32)
                parts = [x_ref[rows, :].astype(f32) for x_ref in x_refs]
                parts.append(halves[part][t * step + r : t * step + r + 32, :].astype(f32))
                total = parts[0]
                for p in parts[1:]:
                    total = total + p
                mean = jnp.sum(total, axis=1, keepdims=True) * (1.0 / D)
                cs = [p - mean for p in parts]
                sq = cs[0] * cs[0]
                for c in cs[1:]:
                    sq = sq + c * c
                var = jnp.sum(sq, axis=1, keepdims=True) * (1.0 / D)
                inv = lax.rsqrt(var + 1e-06)
                for h in range(8):
                    to = slice(part * step + r, part * step + r + 32)
                    n_ref[ids_ref[h], to] = (cs[h] * inv * gain_ref[ids_ref[h]]).astype(bf16)

    def one(t, n_ref):
        normed = jnp.concatenate([n_ref[h] for h in range(8)], axis=1)
        qk = jnp.dot(normed, jnp.concatenate([w_ref[0], w_ref[1]], axis=1), preferred_element_type=f32)
        v = jnp.dot(normed, w_ref[2], preferred_element_type=f32)
        k0, k1 = qk[:step, 128:], qk[step:, 128:]
        first = jnp.where(low, k0, pltpu.roll(k1, HD, 1))
        second = jnp.where(low, pltpu.roll(k0, HD, 1), k1)
        rows = slice(t * step, (t + 1) * step)
        kv_ref[rows, :] = jnp.where(par > 0, second, first).astype(bf16)
        out_ref[rows, :] = jnp.where(par > 0, first, second).astype(bf16)
        for part in range(2):
            own = slice(part * step, (part + 1) * step)
            block = (part * (half // step) + t) * HD
            vt = v[own].T
            vkeep = jnp.where(par > 0, vt[HD:], vt[:HD])
            vgive = jnp.where(par > 0, vt[:HD], vt[HD:])
            to = slice(half + block, half + block + HD)
            kv_ref[to, :] = vkeep.astype(bf16)
            out_ref[to, :] = vgive.astype(bf16)
            qt = (qk[own, :128] * QSCALE).T
            qkeep = jnp.where(par > 0, qt[HD:], qt[:HD])
            qgive = jnp.where(par > 0, qt[:HD], qt[HD:])
            q_ref[block : block + HD, :] = qkeep.astype(bf16)
            qout_ref[block : block + HD, :] = qgive.astype(bf16)

    bufs = (n_even, n_odd)
    trips = half // step
    norm(0, bufs[0])
    for t in range(trips):
        if t + 1 < trips:
            norm(t + 1, bufs[(t + 1) % 2])
        one(t, bufs[t % 2])


def stage_kernel(*refs):
    sems = refs[-1]
    count = len(refs) // 2
    copies = [pltpu.make_async_copy(refs[n], refs[count + n], sems.at[n]) for n in range(count)]
    for c in copies:
        c.start()
    for c in copies:
        c.wait()


def stage(*arrays):
    arrays = [pltpu.with_memory_space_constraint(a, pltpu.HBM) for a in arrays]
    return pl.pallas_call(
        stage_kernel,
        out_shape=[jax.ShapeDtypeStruct(a.shape, a.dtype) for a in arrays],
        in_specs=[hbm() for a in arrays],
        out_specs=[vmem() for a in arrays],
        scratch_shapes=[pltpu.SemaphoreType.DMA((len(arrays),))],
        compiler_params=pltpu.CompilerParams(vmem_limit_bytes=2 << 20),
        name="stage",
    )(*arrays)


def project(ids, blocks, gain, w):
    tok = blocks[0].shape[0]
    return pl.pallas_call(
        project_kernel,
        out_shape=(
            jax.ShapeDtypeStruct((tok, 128), bf16),
            jax.ShapeDtypeStruct((tok // 2, 128), bf16),
            jax.ShapeDtypeStruct((tok, 128), bf16),
            jax.ShapeDtypeStruct((tok // 2, 128), bf16),
        ),
        in_specs=[smem()] + [vmem()] * 11,
        out_specs=(vmem(), vmem(), vmem(), vmem()),
        scratch_shapes=[
            pltpu.VMEM((8, 256, 128), bf16),
            pltpu.VMEM((8, 256, 128), bf16),
        ],
        compiler_params=pltpu.CompilerParams(vmem_limit_bytes=12 << 20),
        name="project",
    )(ids, *blocks, gain, w)


def attend_kernel(*refs, npieces, windows, offset, first, outs, bq, unroll, ahead):
    pieces = refs[:npieces]
    qs = refs[npieces : npieces + len(windows)]
    rest = list(refs[npieces + len(windows) :])
    if not first:
        acc_in, m_in = rest[:2]
        rest = rest[2:]
    out_refs = rest[:outs]
    rest = rest[outs:]
    acc_ref, m_ref, q2, s = rest
    tiles = [(p, r) for p in pieces for r in range(0, p.shape[0], 1024)]
    nkb = len(tiles)
    nqb = q2.shape[0]
    per = bq // 128
    zero = jnp.zeros((HD, bq), bf16)
    jb = 0
    for q, (start, count) in zip(qs, windows):
        for j in range(count // HD // per):
            blocks = [q[start + (j * per + b) * HD : start + (j * per + b + 1) * HD, :] for b in range(per)]
            block = jnp.concatenate(blocks, axis=1)
            q2[jb, 0, 0:HD] = block
            q2[jb, 0, HD:] = zero
            q2[jb, 1, 0:HD] = zero
            q2[jb, 1, HD:] = block
            jb += 1

    if first:
        for j in range(nqb):
            top = jnp.dot(tiles[0][0][0:128], q2[j, 0], preferred_element_type=f32)
            m_ref[j] = jnp.max(top, axis=0, keepdims=True)
    else:
        for j in range(nqb):
            m_ref[j] = m_in[offset + j]

    def reset(j, _):
        acc_ref[j] = jnp.zeros(acc_ref.shape[1:], f32) if first else acc_in[offset + j]
        return 0

    lax.fori_loop(0, nqb, reset, 0)

    blocks = unroll // nkb
    units = [(d, i, c, g) for d in range(blocks) for i in range(nkb) for c in range(4) for g in range(bq // 256)]

    def unit(j, i, c, g):
        piece, row = tiles[i]
        half, at = c // 2, row + (c % 2) * 256
        k = piece[at : at + 256, :]
        return jnp.dot(k, q2[j, half, :, g * 256 : (g + 1) * 256], preferred_element_type=f32)

    def values(i, c):
        piece, row = tiles[i]
        at = [row + 512 + (c * 2 + b) * HD for b in range(2)]
        return jnp.concatenate([piece[r : r + HD, :] for r in at], axis=1)

    def trip(h):
        base = h * blocks
        then = jnp.where(base + blocks < nqb, base + blocks, 0)
        todo = [s[n] for n in range(ahead)]
        order = [(base + d, i, c, g) for d, i, c, g in units[ahead:]]
        order += [(then + d, i, c, g) for d, i, c, g in units[:ahead]]
        state = {}
        for n, (d, i, c, g) in enumerate(units):
            made = unit(*order[n])
            if n < len(units) - ahead:
                todo.append(made)
            else:
                s[n - (len(units) - ahead)] = made
            at = slice(g * 256, (g + 1) * 256)
            if (d, g) not in state:
                state[d, g] = [acc_ref[base + d, :HD, at], acc_ref[base + d, HD:, at], m_ref[base + d, :, at]]
            acc, den, top = state[d, g]
            p = jnp.exp2(todo[n] - top)
            den = den + jnp.sum(p.reshape(32, 8, 256), axis=0)
            acc = acc + jnp.dot(values(i, c), p.astype(bf16), preferred_element_type=f32)
            state[d, g] = [acc, den, top]
            if i == nkb - 1 and c == 3:
                acc_ref[base + d, :HD, at] = acc
                acc_ref[base + d, HD:, at] = den

    def exact(j, _):
        top = jnp.full((1, bq), -jnp.inf, f32) if first else m_in[offset + j]
        for piece, row in tiles:
            for half in range(2):

                def widen(r, top, piece=piece, row=row, half=half):
                    k = piece[pl.ds(pl.multiple_of(row + r * 128, 128), 128), :]
                    part = jnp.dot(k, q2[j, half], preferred_element_type=f32)
                    return jnp.maximum(top, jnp.max(part, axis=0, keepdims=True))

                top = lax.fori_loop(0, 4, widen, top)
        if first:
            acc_ref[j] = jnp.zeros(acc_ref.shape[1:], f32)
        else:
            acc_ref[j] = acc_in[offset + j] * jnp.exp2(m_in[offset + j] - top)
        m_ref[j] = top
        return 0

    def sweep(turn):
        @pl.when(turn > 0)
        def _():
            lax.fori_loop(0, nqb, exact, 0)

        for n in range(ahead):
            s[n] = unit(*units[n])

        def some(h, _):
            trip(h)
            return 0

        lax.fori_loop(0, nqb // blocks, some, 0)
        den = acc_ref[:, HD:, :]
        fine = jnp.min(jnp.where(den < CAP, 1.0, 0.0)) > 0.5
        return jnp.where(jnp.logical_or(turn > 0, fine), 2, 1)

    lax.while_loop(lambda turn: turn < 2, sweep, 0)

    for n, out_ref in enumerate(out_refs):
        for j in range(nqb // outs):
            a = acc_ref[n * (nqb // outs) + j]
            o = (a[0:HD] * (1.0 / jnp.sum(a[HD:], axis=0, keepdims=True))).astype(bf16)
            for b in range(per):
                out_ref[(j * per + b) * HD : (j * per + b + 1) * HD, :] = o[:, b * 128 : (b + 1) * 128]


def attend(pieces, qs, state=None, offset=0, outs=0, bq=512, unroll=8, ahead=4):
    windows = tuple(w for q, w in qs)
    nkeys = sum(p.shape[0] for p in pieces)
    nqueries = sum(count for start, count in windows) * 2
    nqb = nqueries // bq
    acc_shape = (nqb, HD + 8, bq)
    m_shape = (nqb, 1, bq)
    scratch = [
        pltpu.VMEM((nqb, 2, 128, bq), bf16),
        pltpu.VMEM((max(ahead, 1), 256, 256), f32),
    ]
    if outs:
        out_shape = [jax.ShapeDtypeStruct((nqueries // 2 // outs, 128), bf16)] * outs
        out_specs = [vmem()] * outs
        scratch = [pltpu.VMEM(acc_shape, f32), pltpu.VMEM(m_shape, f32)] + scratch
    else:
        out_shape = (jax.ShapeDtypeStruct(acc_shape, f32), jax.ShapeDtypeStruct(m_shape, f32))
        out_specs = (vmem(), vmem())
    args = [*pieces, *(q for q, w in qs)] + ([] if state is None else list(state))
    flops = 4 * nkeys * nqueries * 128
    return pl.pallas_call(
        functools.partial(
            attend_kernel, npieces=len(pieces), windows=windows, offset=offset, first=state is None, outs=outs, bq=bq, unroll=unroll, ahead=ahead
        ),
        out_shape=out_shape,
        in_specs=[vmem()] * len(args),
        out_specs=out_specs,
        scratch_shapes=scratch,
        compiler_params=pltpu.CompilerParams(vmem_limit_bytes=16 << 20),
        cost_estimate=pl.CostEstimate(flops=flops, transcendentals=nkeys * nqueries, bytes_accessed=nkeys * 256),
    )(*args)


def columns_of(att_refs, t, swap):
    kept, back, peer_kept, peer_back = att_refs
    at = pl.ds(pl.multiple_of(t * HD, HD), HD)
    cols = []
    for mine, other in ((kept, back), (peer_kept, peer_back)):
        a, b = mine[at, :], other[at, :]
        cols += [jnp.where(swap, b, a), jnp.where(swap, a, b)]
    return jnp.concatenate(cols, axis=0).T


def weights_for(pos_ref, own_ref, peer_ref, w_ref, steps):
    for n, b in enumerate(steps):
        cols = pl.ds(pl.multiple_of((((pos_ref[0] + b) % 4) * 2 + pos_ref[1]) * 128, 128), 128)
        w_ref[0:128, n * 128 : (n + 1) * 128] = own_ref[:, cols]
        w_ref[128:256, n * 128 : (n + 1) * 128] = peer_ref[:, cols]


def far_kernel(pos_ref, *refs):
    att_refs, (own_ref, peer_ref, lo_ref, hi_ref, t_ref, w_ref) = refs[:4], refs[4:]
    weights_for(pos_ref, own_ref, peer_ref, w_ref, (2,))
    swap = pos_ref[2] > 0
    count = att_refs[0].shape[0] // HD
    for t in range(count):
        rows = columns_of(att_refs, t, swap)
        t_ref[t] = rows
        out = jnp.dot(rows, w_ref[...], preferred_element_type=f32).astype(bf16)
        half = (lo_ref, hi_ref)[t // (count // 2)]
        to = (t % (count // 2)) * 128
        half[to : to + 128, :] = out


def mix_far(pos, att, own, peer):
    tok = att[0].shape[0] * 2
    return pl.pallas_call(
        far_kernel,
        out_shape=[jax.ShapeDtypeStruct((tok // 2, 128), bf16)] * 2
        + [jax.ShapeDtypeStruct((tok // 128, 128, 256), bf16)],
        in_specs=[smem()] + [vmem()] * 6,
        out_specs=[vmem()] * 3,
        scratch_shapes=[pltpu.VMEM((256, 128), bf16)],
        compiler_params=pltpu.CompilerParams(vmem_limit_bytes=6 << 20),
        name="mix_far",
    )(pos, *att, own, peer)


def mix_kernel(pos_ref, rows_ref, own_ref, peer_ref, x_ref, bias_ref, base_ref, up_ref, down_ref, w_ref):
    weights_for(pos_ref, own_ref, peer_ref, w_ref, (0, 1, 3))

    def one(t, _):
        out = jnp.dot(rows_ref[t], w_ref[...], preferred_element_type=f32)
        to = pl.ds(pl.multiple_of(t * 128, 128), 128)
        base_ref[to, :] = out[:, :128] + x_ref[to, :].astype(f32) + bias_ref[...]
        up_ref[to, :] = out[:, 128:256].astype(bf16)
        down_ref[to, :] = out[:, 256:].astype(bf16)
        return 0

    lax.fori_loop(0, rows_ref.shape[0], one, 0, unroll=4)


def mix(pos, rows, own, peer, x, bias):
    return pl.pallas_call(
        mix_kernel,
        out_shape=[jax.ShapeDtypeStruct(x.shape, f32)] + [jax.ShapeDtypeStruct(x.shape, bf16)] * 2,
        in_specs=[smem()] + [vmem()] * 5,
        out_specs=[vmem()] * 3,
        scratch_shapes=[pltpu.VMEM((256, 384), bf16)],
        compiler_params=pltpu.CompilerParams(vmem_limit_bytes=6 << 20),
        name="mix",
    )(pos, rows, own, peer, x, bias)


def join_kernel(up_ref, down_ref, lo_ref, hi_ref, upo_ref, downo_ref):
    half = lo_ref.shape[0]
    upo_ref[:half] = (up_ref[:half].astype(f32) + lo_ref[...].astype(f32)).astype(bf16)
    upo_ref[half:] = up_ref[half:]
    downo_ref[:half] = down_ref[:half]
    downo_ref[half:] = (down_ref[half:].astype(f32) + hi_ref[...].astype(f32)).astype(bf16)


def join(up, down, lo, hi):
    return pl.pallas_call(
        join_kernel,
        out_shape=[jax.ShapeDtypeStruct(up.shape, bf16)] * 2,
        in_specs=[vmem()] * 4,
        out_specs=[vmem()] * 2,
        compiler_params=pltpu.CompilerParams(vmem_limit_bytes=6 << 20),
        name="join",
    )(up, down, lo, hi)


def per_device(tokens, ln_gain, w_qkv, w_out, out_bias):
    rows = lax.axis_index("rows")
    heads = lax.axis_index("heads")
    yh = rows // 2
    x = heads // 2
    yl = heads % 2
    tok = tokens.shape[0]

    by_y = send(tokens, YL_SWAP)
    by_up = send(tokens, X_UP)
    by_down = send(tokens, X_DOWN)
    y_up = send(by_up, YL_SWAP)
    y_down = send(by_down, YL_SWAP)
    y_far = send(by_y, X_FAR)
    far_lo = send(by_up[: tok // 2], X_UP)
    far_hi = send(by_down[tok // 2 :], X_DOWN)
    held, w_held, bias = stage(tokens, w_qkv, out_bias.reshape(1, 128))
    blocks = (held, by_up, by_down, by_y, y_up, y_down, y_far, far_lo, far_hi)
    xs = jnp.stack([x, (x + 3) % 4, (x + 1) % 4, (x + 2) % 4])
    ids = jnp.concatenate([xs[:3] * 2 + yl, xs * 2 + 1 - yl, xs[3:] * 2 + yl, yh.reshape(1)]).astype(jnp.int32)

    kv, q, give, give_q = project(ids, blocks, ln_gain.reshape(8, 1, 128), w_held)
    kf = send(give, YH_SWAP)
    q_far = send(give_q, YH_SWAP)
    k_other = send(kv, CORE_SWAP)
    k_up = send(kv, Z_UP)
    k_down = send(kv, Z_DOWN)
    f_other = send(kf, CORE_SWAP)
    f_up = send(kf, Z_UP)
    f_down = send(kf, Z_DOWN)
    qs = ((q_far, (0, tok // 2)), (q, (0, tok // 2)))
    state = attend((kv, kf, k_other, f_other), qs)
    k_up, k_down, f_up, f_down, w_send, state = lax.optimization_barrier((k_up, k_down, f_up, f_down, w_out, state))
    chosen = jnp.where(rows % 2 > 0, jnp.stack([k_down, f_down]), jnp.stack([k_up, f_up]))
    far = send(chosen.reshape(2 * tok, 128), Z_BY_CORE)
    ring = (k_up, k_down, f_up, f_down)
    ring = ring + tuple(send(p, CORE_SWAP) for p in ring)
    w_peer = send(w_send, YL_SWAP)
    state_far = attend(ring, qs[:1], state)
    ends = (far, send(far, CORE_SWAP))
    (att_far,) = attend(ends, qs[:1], state_far, outs=1)
    back = send(att_far, YH_SWAP)
    q_own, att_far = lax.optimization_barrier((q, att_far))
    qs_own = ((q_own, (0, tok // 2)),)
    state_own = attend(ring, qs_own, state, offset=2)
    peer_back = send(back, YL_SWAP)
    (att,) = attend(ends, qs_own, state_own, outs=1)
    peer = send(att, YL_SWAP)
    pos = jnp.stack([x, yl, yh]).astype(jnp.int32)
    lo, hi, att_rows = mix_far(pos, (att, back, peer, peer_back), w_out, w_peer)
    lo = send(lo, X_UP)
    hi = send(hi, X_DOWN)
    base, up, down = mix(pos, att_rows, w_out, w_peer, tokens, bias)
    up, down = join(up, down, lo, hi)
    up = send(up, X_UP)
    down = send(down, X_DOWN)
    return (base + up.astype(f32) + down.astype(f32)).astype(bf16)


def solution(mesh):
    return jax.shard_map(
        per_device,
        mesh=mesh,
        in_specs=(
            P(("rows", "cols"), "heads"),
            P(),
            P(None, None, "heads"),
            P("heads", None),
            P("heads"),
        ),
        out_specs=P(("rows", "cols"), "heads"),
        check_vma=False,
    )
```
